32 devices in a mesh: dp: 16 (over z, x, core), tensor: 2 (over y).
Axes of the slice: x: 2, y: 2, z: 4, core: 2. Of those that a mesh axis runs over, the one named last changes fastest.
Arguments:
- pixels: bfloat16 [32, 256, 768], P('dp'), may hold values from 0.03 to 4.4
- lengths: int32 [32], P('dp'), may hold values from 1 to 256, 6144 in all
- patch_ids: int32 [32, 256], P('dp'), may hold values from 0 to 783, as said below
- gsd_values: int32 [32], P('dp'), may hold values from 30 to 300
- embed_w: bfloat16 [768, 1024], replicated, may hold values from -0.21875 to 0.21875
- embed_bias: float32 [1024], replicated, may hold values from -1.5 to 1.5
- norm_gain: float32 [2, 1024], replicated, may hold values from 0.25 to 1.75
- norm_bias: float32 [2, 1024], replicated, may hold values from -1.5 to 1.5
- qkv_w: bfloat16 [3, 1024, 1024], P(None, None, 'tensor'), may hold values from -0.1875 to 0.1875
- qv_bias: float32 [2, 1024], P(None, 'tensor'), may hold values from -1.5 to 1.5
- out_w: bfloat16 [1024, 1024], P('tensor'), may hold values from -1 to 1
- out_bias: float32 [1024], replicated, may hold values from -1.5 to 1.5
- up_w: bfloat16 [1024, 4096], P(None, 'tensor'), may hold values from -0.1875 to 0.1875
- up_bias: float32 [4096], P('tensor'), may hold values from -2.5 to 2.5
- down_w: bfloat16 [4096, 1024], P('tensor'), may hold values from -0.09375 to 0.09375
- down_bias: float32 [1024], replicated, may hold values from -1.5 to 1.5
- cotangent: bfloat16 [32, 256, 1024], P('dp'), may hold values from -6 to 6
Outputs:
- output: bfloat16 [32, 256, 1024], P('dp')
- pixel_grad: float32 [32, 256, 768], P('dp')
- grad_embed: float32 [768, 1024], replicated
- grad_embed_bias: float32 [1024], replicated
- grad_norm_gain: float32 [2, 1024], replicated
- grad_norm_bias: float32 [2, 1024], replicated
- grad_qkv: float32 [3, 1024, 1024], P(None, None, 'tensor')
- grad_qv_bias: float32 [2, 1024], P(None, 'tensor')
- grad_out_proj: float32 [1024, 1024], P('tensor')
- grad_out_bias: float32 [1024], replicated
- grad_up: float32 [1024, 4096], P(None, 'tensor')
- grad_up_bias: float32 [4096], P('tensor')
- grad_down: float32 [4096, 1024], P('tensor')
- grad_down_bias: float32 [1024], replicated
The draws below stay inside these ranges and needn't reach their ends.
Inputs may be any that keep to these rules, and one draw needn't show every extreme that they name: `patch_ids`: each row holds 256 distinct patch numbers of a 28 by 28 grid. `lengths`: the longest image has exactly 256 visible patches.
All inputs are finite; a program needn't handle non-finite values. No bound on the sum of `lengths` on one device may be relied on, other than what follows from the above.
Results may differ from the reference program's by a relative error of at most 0.013.
The reference program's roundings to bfloat16 on the way count: a program that leaves them out, or rounds other values in their place, can miss the bound.
Values sent between devices are 32-bit elements; how exact they have to be, the bound alone decides.
A program may use at most 192 MiB of HBM per device.

```python
import math
import jax
import jax.numpy as jnp
import numpy as np
from jax import lax

D = 1024
HEADS = 16
HD = 64
FF = 4096
PATCH = 16
GRID = 28
CAP = 256
PATCH_DIM = 768
IMAGES = 32


def draw_pixels(key, part):
    band_key, noise_key = jax.random.split(key, 2)
    image_ramp = jnp.arange(IMAGES, dtype=jnp.float32) / (IMAGES - 1)
    band_factor = jnp.exp(jax.random.uniform(band_key, (IMAGES, 1, 3, 1), jnp.float32, -0.3, 0.3))
    image_level = 0.3 * (1.0 + 2.0 * image_ramp)
    pixel_noise = jnp.clip(0.4 * jax.random.normal(noise_key, (IMAGES, CAP, 3, PATCH * PATCH), jnp.float32), -0.8, 0.8)
    values = image_level[:, None, None, None] * band_factor * (1.0 + pixel_noise)
    return values.reshape(IMAGES, CAP, 3 * PATCH * PATCH).astype(jnp.bfloat16)


def draw_patch_ids(key, part):
    image_keys = jax.random.split(key, IMAGES)

    def one_image(image_key):
        return jax.random.permutation(image_key, GRID * GRID)[:CAP].astype(jnp.int32)
    return jax.vmap(one_image)(image_keys)


def plant(entries, key, smallest, high):
    shape = entries.shape
    place = [jax.random.randint(jax.random.fold_in(key, axis), (), 0, shape[axis]) for axis in range(len(shape))]
    entries = entries.at[tuple(place)].set(smallest)
    longest = shape.index(max(shape))
    place[longest] = (place[longest] + 1) % shape[longest]
    return entries.at[tuple(place)].set(high)


def block_scale(rng, extent, cuts, smallest, largest):
    factor_of, own = 1.0, jax.random.fold_in(rng, 6)
    for axis_at, parts in cuts:
        steps = jnp.exp(jax.random.uniform(jax.random.fold_in(own, axis_at), (parts,), jnp.float32, smallest / len(cuts), largest / len(cuts)))
        factor_of = factor_of * jnp.repeat(steps, extent[axis_at] // parts).reshape([-1 if axis == axis_at else 1 for axis in range(len(extent))])
    return factor_of


def profile(amount, total, reach, skew):
    portions = [(1 << 20) // math.isqrt(standing ** skew) + 1 for standing in range(2, amount + 1)]
    surplus, holding = total - reach - (amount - 1), [1] * (amount - 1)
    while surplus > 0:
        free = [i for i in range(amount - 1) if holding[i] < reach]
        pool, left = sum([portions[i] for i in free]), surplus
        for i in free:
            more = min(reach - holding[i], max(1, left * portions[i] // pool), surplus)
            holding[i] = holding[i] + more
            surplus = surplus - more
    return np.array([reach] + holding)


def uneven(own_key, number_of, total, reach, skew):
    if number_of == 2:
        one = jax.random.randint(own_key, (), max(1, total - reach), min(reach, total - 1) + 1)
        return jnp.stack([one, total - one])
    sizes = jnp.asarray(profile(number_of, total, reach, skew), jnp.int32)
    pairs = (number_of - 1) // 2
    donor, taker = sizes[1:1 + 2 * pairs:2], sizes[2:2 + 2 * pairs:2]
    margin = jnp.minimum(donor - 1, reach - taker)
    moved = jax.random.randint(jax.random.fold_in(own_key, 1), (pairs,), 0, 1 << 20) % (margin + 1)
    sizes = sizes.at[1:1 + 2 * pairs:2].set(donor - moved).at[2:2 + 2 * pairs:2].set(taker + moved)
    return sizes[jax.random.permutation(jax.random.fold_in(own_key, 2), number_of)]


def scatter_about(stream_key, dims, width, reach, shards=(), kind=jnp.bfloat16):
    array = width * jax.random.normal(stream_key, dims, jnp.float32)
    if shards:
        array = array * block_scale(stream_key, dims, shards, -0.22, 0.18)
    return jnp.clip(array, -reach, reach).astype(kind)


def setup_inputs(seed: int = 0) -> dict:
    splits = jax.random.split(jax.random.key(seed), 18)
    pixels = draw_pixels(jax.random.fold_in(splits[17], 71), 0)
    lengths = uneven(splits[1], IMAGES, IMAGES * 3 * CAP // 4, CAP, 2).astype(jnp.int32)
    patch_ids = draw_patch_ids(jax.random.fold_in(splits[17], 71), 0)
    gsd_values = plant(jax.random.randint(splits[3], (IMAGES,), 30, 301), jax.random.fold_in(splits[3], 1), 30, 300).astype(jnp.int32)
    embed_w = scatter_about(splits[4], (PATCH_DIM, D), PATCH_DIM ** -0.5, 0.21875)
    embed_bias = scatter_about(splits[5], (D,), 0.3, 1.5, (), jnp.float32)
    norm_gain = jnp.clip(1.0 + 0.15 * jax.random.normal(splits[6], (2, D), jnp.float32), 0.25, 1.75)
    norm_bias = scatter_about(splits[7], (2, D), 0.3, 1.5, (), jnp.float32)
    qkv_w = scatter_about(splits[8], (3, D, D), D ** -0.5, 0.1875, ((2, 2),))
    qv_bias = scatter_about(splits[9], (2, D), 0.3, 1.5, ((1, 2),), jnp.float32)
    out_w = scatter_about(splits[10], (D, D), (max(D // 32, 1)) ** -0.5, 1.0, ((0, 2),))
    out_bias = scatter_about(splits[11], (D,), 0.3, 1.5, (), jnp.float32)
    up_w = scatter_about(splits[12], (D, FF), D ** -0.5, 0.1875, ((1, 2),))
    up_bias = scatter_about(splits[13], (FF,), 0.5, 2.5, ((0, 2),), jnp.float32)
    down_w = scatter_about(splits[14], (FF, D), FF ** -0.5, 0.09375, ((0, 2),))
    down_bias = scatter_about(splits[15], (D,), 0.3, 1.5, (), jnp.float32)
    cotangent = scatter_about(splits[16], (IMAGES, CAP, D), 1.0, 6.0, ((0, 16),))
    return {"pixels": pixels, "lengths": lengths, "patch_ids": patch_ids, "gsd_values": gsd_values, "embed_w": embed_w, "embed_bias": embed_bias, "norm_gain": norm_gain, "norm_bias": norm_bias, "qkv_w": qkv_w, "qv_bias": qv_bias, "out_w": out_w, "out_bias": out_bias, "up_w": up_w, "up_bias": up_bias, "down_w": down_w, "down_bias": down_bias, "cotangent": cotangent}


@jax.custom_vjp
def low(v):
    return lax.optimization_barrier(v.astype(jnp.bfloat16)).astype(jnp.float32)

@jax.custom_vjp
def low_back(v):
    return v

def low_keep(v):
    return (low(v), None)

def low_pass(kept, grad):
    return (grad,)

def back_keep(v):
    return (v, None)

def back_low(kept, grad):
    return (low(grad),)
low.defvjp(low_keep, low_pass)
low_back.defvjp(back_keep, back_low)

def matmul(left_side, right_side):
    return jnp.dot(left_side, right_side, precision=lax.Precision.HIGHEST, preferred_element_type=jnp.float32)

def positions(patch_ids, gsd_values, model_width, grid_side):
    quarter = model_width // 4
    gsd_scale = gsd_values.astype(jnp.float32) / 100.0
    row_pos = (patch_ids // grid_side).astype(jnp.float32) * gsd_scale[:, None]
    col_pos = (patch_ids % grid_side).astype(jnp.float32) * gsd_scale[:, None]
    frequency = jnp.exp(jnp.arange(quarter, dtype=jnp.float32) * (-math.log(10000.0) / quarter))
    row_angle = row_pos[:, :, None] * frequency
    col_angle = col_pos[:, :, None] * frequency
    return jnp.concatenate([jnp.sin(row_angle), jnp.cos(row_angle), jnp.sin(col_angle), jnp.cos(col_angle)], axis=-1)

def layer_norm(hidden, gain_row, shift_row):
    centred = hidden - lax.optimization_barrier(jnp.mean(hidden, axis=-1, keepdims=True))
    inverse = lax.rsqrt(lax.optimization_barrier(jnp.mean(centred * centred, axis=-1, keepdims=True)) + 1e-06)
    return centred * inverse * gain_row + shift_row

def attend(queries, key_rows, values, key_keep):
    score_scale = 1.0 / math.sqrt(queries.shape[-1])
    scores = jnp.einsum('ichd,ijhd->ihcj', queries, key_rows, precision=lax.Precision.HIGHEST) * score_scale
    scores = low_back(scores)
    scores = jnp.where(key_keep[:, None, None, :], scores, -1e+30)
    top_score = lax.optimization_barrier(jnp.max(scores, axis=-1, keepdims=True))
    exp_scores = jnp.exp(scores - top_score)
    attn_probs = exp_scores / lax.optimization_barrier(jnp.sum(exp_scores, axis=-1, keepdims=True))
    return jnp.einsum('ihcj,ijhd->ichd', low(attn_probs), values, precision=lax.Precision.HIGHEST)

def forward(pixel_vals, embed_w, embed_bias, norm_gain, norm_bias, qkv_w, qv_bias, out_w, out_bias, up_w, up_bias, down_w, down_bias, valid_rows, key_keep, pos_table):
    images, slot_count, patch_width = pixel_vals.shape
    band_width = patch_width // 3
    pixel_grid = pixel_vals.reshape(images, slot_count, 3, band_width)
    pixel_mask = valid_rows[:, :, None, None]
    band_count = jnp.sum(valid_rows) * band_width
    band_mean = lax.optimization_barrier(jnp.sum(pixel_grid * pixel_mask, axis=(0, 1, 3))) / band_count
    band_rstd = lax.rsqrt(lax.optimization_barrier(jnp.sum(pixel_grid * pixel_grid * pixel_mask, axis=(0, 1, 3))) / band_count - band_mean * band_mean + 1e-05)
    pixel_hat = ((pixel_grid - band_mean[:, None]) * band_rstd[:, None]).reshape(images * slot_count, patch_width)
    stream_zero = low_back(matmul(low(pixel_hat), embed_w)) + embed_bias + pos_table
    attn_input = low(layer_norm(stream_zero, norm_gain[0], norm_bias[0]))
    queries = low(low_back(matmul(attn_input, qkv_w[0]) + qv_bias[0]))
    key_rows = low(low_back(matmul(attn_input, qkv_w[1])))
    values = low(low_back(matmul(attn_input, qkv_w[2]) + qv_bias[1]))
    group_size = math.gcd(images, 16)

    def to_groups(flat_rows):
        return flat_rows.reshape(images // group_size, group_size, slot_count, HEADS, HD)
    checked = jax.checkpoint(attend)
    attended = lax.map(lambda block_in: checked(*block_in), (to_groups(queries), to_groups(key_rows), to_groups(values), key_keep.reshape(images // group_size, group_size, slot_count)))
    attended = low(low_back(attended.reshape(images * slot_count, HEADS * HD)))
    stream_one = stream_zero + low_back(matmul(attended, out_w)) + out_bias
    mlp_input = low(layer_norm(stream_one, norm_gain[1], norm_bias[1]))
    hidden_pre = low_back(matmul(mlp_input, up_w) + up_bias)
    hidden_low = low(jax.nn.gelu(hidden_pre, approximate=False))
    stream_two = stream_one + low_back(matmul(hidden_low, down_w)) + down_bias
    return (stream_two * valid_rows.reshape(-1, 1)).reshape(images, slot_count, -1)

def reference(pixels, lengths, patch_ids, gsd_values, embed_w, embed_bias, norm_gain, norm_bias, qkv_w, qv_bias, out_w, out_bias, up_w, up_bias, down_w, down_bias, cotangent):
    slot_count = pixels.shape[1]
    key_keep = jnp.arange(slot_count)[None, :] < lengths[:, None]
    valid_rows = key_keep.astype(jnp.float32)
    pos_table = positions(patch_ids, gsd_values, D, GRID).reshape(-1, D)
    params = tuple((source.astype(jnp.float32) for source in (pixels, embed_w, embed_bias, norm_gain, norm_bias, qkv_w, qv_bias, out_w, out_bias, up_w, up_bias, down_w, down_bias)))

    def closed(*inputs):
        return forward(*inputs, valid_rows, key_keep, pos_table)
    primal, pullback = jax.vjp(closed, *params)
    gradients = pullback(cotangent.astype(jnp.float32))
    return (primal.astype(jnp.bfloat16), gradients[0], gradients[1], gradients[2], gradients[3], gradients[4], gradients[5], gradients[6], gradients[7], gradients[8], gradients[9], gradients[10], gradients[11], gradients[12])
```

```python
import functools
import math

import jax
import jax.numpy as jnp
from jax import lax
from jax.experimental import pallas as pl
from jax.experimental.pallas import tpu as pltpu
from jax.sharding import PartitionSpec as P

HD = 64
GRID = 28
MESH = pl.DeviceIdType.MESH
W = 512


SEND = ("c","x","oa","ob","ja","jb","xb","ga","gb","na","fa","nb","fb","xg","cg")

def dp_kernel(shapes, R, K, delays, *refs):
    n = len(shapes)
    ins, outs = refs[:n], refs[n:2*n]
    own, cl, xl, ab, oa, ob, ja, jb, nbuf, xbl, fin, ssem, rsem, lsem = refs[2*n:]
    H, Q, E = R//2, R//4, R//8
    i = lax.axis_index("dp"); t = lax.axis_index("tensor")
    c = lax.rem(i, 2); x = lax.rem(i//2, 2); z = i//4
    side = z//2
    pos = lax.rem(z, 2)
    inner = lax.rem(side + pos, 2) == 1
    outer = lax.rem(side + pos, 2) == 0
    dev_c = (z*4 + x*2 + 1 - c, t)
    dev_x = (z*4 + (1-x)*2 + c, t)
    dev_o = ((side*2 + 1 - pos)*4 + x*2 + c, t)
    dev_j = ((3 - z)*4 + x*2 + c, t)
    bar = pltpu.get_barrier_semaphore()
    for d in (dev_c, dev_x, dev_o):
        pl.semaphore_signal(bar, inc=1, device_id=d, device_id_type=MESH)
    @pl.when(inner)
    def _():
        pl.semaphore_signal(bar, inc=1, device_id=dev_j, device_id_type=MESH)
        pl.semaphore_wait(bar, 4)
    @pl.when(outer)
    def _():
        pl.semaphore_wait(bar, 3)
    starts, total = [], 0
    for (rows, cols) in shapes:
        starts.append(total); total += (rows//(2*R))*(cols//W)
    NC = total
    def al(v, m): return pl.multiple_of(v, m)
    def slot(j): return lax.rem(j, K)
    a_mine = al(x*Q, Q); a_other = al((1-x)*Q, Q)
    e_near = al(side*E, E); e_far = al((1-side)*E, E)
    b_near = al(H + side*Q, Q); b_far = al(H + (1-side)*Q, Q)
    aN = al(x*Q + side*E, E); aF = al(x*Q + (1-side)*E, E)
    def hbm(ref, a, j, half):
        cols = shapes[a][1]//W
        q = j - starts[a]
        r = al((q//cols)*(2*R) + half*R, R)
        col = al(lax.rem(q, cols)*W, W)
        return ref.at[pl.ds(r, R), pl.ds(col, W)]
    def rc(kind, src, dst, dev, s):
        k = SEND.index(kind)
        return pltpu.make_async_remote_copy(src_ref=src, dst_ref=dst, send_sem=ssem.at[k, s], recv_sem=rsem.at[k, s], device_id=dev, device_id_type=MESH)
    def desc(kind, j):
        s = slot(j)
        if kind == "x": return rc(kind, own.at[s, pl.ds(a_other, Q)], xl.at[s], dev_x, s)
        if kind == "ob": return rc(kind, own.at[s, pl.ds(H, H)], ob.at[s], dev_o, s)
        if kind == "oa": return rc(kind, ab.at[s], oa.at[s], dev_o, s)
        if kind == "ja": return rc(kind, ab.at[s, pl.ds(e_far, E)], ja.at[s], dev_j, s)
        if kind == "jb": return rc(kind, own.at[s, pl.ds(b_far, Q)], jb.at[s], dev_j, s)
        if kind == "xb": return rc(kind, nbuf.at[s], xbl.at[s], dev_x, s)
        if kind in ("ga", "na"):
            return rc(kind, fin.at[s, pl.ds(aN, E)], fin.at[s, pl.ds(aN, E)], dev_j if kind == "ga" else dev_o, s)
        if kind == "fa": return rc(kind, fin.at[s, pl.ds(aF, E)], fin.at[s, pl.ds(aF, E)], dev_o, s)
        if kind in ("gb", "nb"):
            return rc(kind, fin.at[s, pl.ds(b_near, Q)], fin.at[s, pl.ds(b_near, Q)], dev_j if kind == "gb" else dev_o, s)
        if kind == "fb": return rc(kind, fin.at[s, pl.ds(b_far, Q)], fin.at[s, pl.ds(b_far, Q)], dev_o, s)
        if kind == "xg": return rc(kind, fin.at[s, pl.ds(a_mine, Q)], fin.at[s, pl.ds(a_mine, Q)], dev_x, s)
        if kind == "c": return rc(kind, hbm(ins[0], 0, starts[0], 1 - c), cl.at[s], dev_c, s)
        if kind == "cg": return rc(kind, fin.at[s], hbm(outs[0], 0, starts[0], c), dev_c, s)
        raise ValueError(kind)
    def each(j, f):
        for a in range(n):
            end = starts[a+1] if a + 1 < n else NC
            if n == 1: f(a); continue
            cond = (j >= starts[a]) & (j < end)
            pl.when(cond)(functools.partial(f, a))
    d = delays
    def step(tt, carry):
        js = [tt - dd for dd in d]
        def on(k): return (js[k] >= 0) & (js[k] < NC)
        @pl.when(on(7))
        def _():
            j = js[7]; s = slot(j)
            pltpu.make_async_copy(fin.at[s], hbm(outs[0], 0, starts[0], c), lsem.at[1, s]).wait()
            desc("cg", j).wait_send(); desc("cg", j).wait_recv()
            desc("c", j).wait_send(); desc("x", j).wait_send(); desc("xg", j).wait_send()
            @pl.when(outer)
            def _():
                desc("oa", j).wait_send(); desc("ob", j).wait_send()
            @pl.when(inner)
            def _():
                for k in ("ja","jb","xb","ga","gb","na","fa","nb","fb"): desc(k, j).wait_send()
        @pl.when(on(6))
        def _():
            j = js[6]
            desc("xg", j).wait_recv()
            @pl.when(outer)
            def _():
                desc("nb", j).wait_recv(); desc("fb", j).wait_recv()
        @pl.when(on(5))
        def _():
            j = js[5]
            @pl.when(inner)
            def _():
                desc("ga", j).wait_recv(); desc("gb", j).wait_recv()
        j5o = tt - d[5] - d[8]
        on5o = (j5o >= 0) & (j5o < NC)
        @pl.when(on5o & outer)
        def _():
            desc("na", j5o).wait_recv(); desc("fa", j5o).wait_recv()
        @pl.when(on(4))
        def _():
            j = js[4]; s = slot(j)
            @pl.when(inner)
            def _():
                desc("ja", j).wait_recv(); desc("xb", j).wait_recv()
                fin[s, pl.ds(aN, E)] = ab[s, pl.ds(e_near, E)] + ja[s]
                fin[s, pl.ds(b_near, Q)] = nbuf[s] + xbl[s]
        @pl.when(on(3))
        def _():
            j = js[3]; s = slot(j)
            @pl.when(inner)
            def _():
                desc("oa", j).wait_recv(); desc("jb", j).wait_recv()
                ab[s] = ab[s] + oa[s]
                nbuf[s] = own[s, pl.ds(b_near, Q)] + jb[s]
        @pl.when(on(2))
        def _():
            j = js[2]; s = slot(j)
            desc("x", j).wait_recv()
            ab[s] = own[s, pl.ds(a_mine, Q)] + xl[s]
            @pl.when(inner)
            def _():
                desc("ob", j).wait_recv()
                own[s, pl.ds(H, H)] = own[s, pl.ds(H, H)] + ob[s]
        @pl.when(on(1))
        def _():
            j = js[1]; s = slot(j)
            pltpu.make_async_copy(hbm(ins[0], 0, starts[0], c), own.at[s], lsem.at[0, s]).wait()
            desc("c", j).wait_recv()
            own[s] = own[s] + cl[s]
        @pl.when(on(6))
        def _():
            j = js[6]; s = slot(j)
            def f(a):
                pltpu.make_async_copy(fin.at[s], hbm(outs[a], a, j, c), lsem.at[1, s]).start()
                rc("cg", fin.at[s], hbm(outs[a], a, j, c), dev_c, s).start()
            each(j, f)
        @pl.when(on(5))
        def _():
            j = js[5]
            @pl.when(inner)
            def _():
                desc("fa", j).start(); desc("xg", j).start(); desc("fb", j).start()
        @pl.when(on5o & outer)
        def _():
            desc("xg", j5o).start()
        @pl.when(on(4))
        def _():
            j = js[4]
            @pl.when(inner)
            def _():
                for k in ("ga","na","gb","nb"): desc(k, j).start()
        @pl.when(on(3))
        def _():
            j = js[3]
            @pl.when(inner)
            def _():
                desc("ja", j).start(); desc("xb", j).start()
        @pl.when(on(2))
        def _():
            j = js[2]
            @pl.when(outer)
            def _(): desc("oa", j).start()
            @pl.when(inner)
            def _(): desc("jb", j).start()
        @pl.when(on(1))
        def _():
            j = js[1]
            desc("x", j).start()
            @pl.when(outer)
            def _(): desc("ob", j).start()
        @pl.when(on(0))
        def _():
            j = js[0]; s = slot(j)
            def f(a):
                pltpu.make_async_copy(hbm(ins[a], a, j, c), own.at[s], lsem.at[0, s]).start()
                rc("c", hbm(ins[a], a, j, 1 - c), cl.at[s], dev_c, s).start()
            each(j, f)
        return carry
    lax.fori_loop(0, NC + d[7], step, 0)

def dp_sum(arrays, R=64, K=16, delays=(0,1,3,5,7,9,12,13,1), name="dp_sum", cid=1):
    shapes = tuple(a.shape for a in arrays)
    n = len(arrays)
    H, Q, E = R//2, R//4, R//8
    f32 = jnp.float32
    V = lambda r: pltpu.VMEM((K, r, W), f32)
    return pl.pallas_call(
        functools.partial(dp_kernel, shapes, R, K, delays),
        out_shape=[jax.ShapeDtypeStruct(s, f32) for s in shapes],
        in_specs=[pl.BlockSpec(memory_space=pl.ANY)]*n,
        out_specs=[pl.BlockSpec(memory_space=pl.ANY)]*n,
        scratch_shapes=[V(R), V(R), V(Q), V(Q), V(Q), V(H), V(E), V(Q), V(Q), V(Q), V(R),
            pltpu.SemaphoreType.DMA((len(SEND), K)), pltpu.SemaphoreType.DMA((len(SEND), K)), pltpu.SemaphoreType.DMA((2, K))],
        compiler_params=pltpu.CompilerParams(collective_id=cid, has_side_effects=True, vmem_limit_bytes=40 << 20),
        name=name)(*arrays)


def stats_kernel(ranks, band_width, lens, pix, out, mine, table, ssem, rsem):
    me = lax.axis_index("dp")
    t = lax.axis_index("tensor")
    bar = pltpu.get_barrier_semaphore()
    for k in range(1, ranks):
        pl.semaphore_signal(bar, inc=1, device_id=(lax.rem(me + k, ranks), t), device_id_type=MESH)
    images, slots, width = pix.shape
    one = jnp.zeros((1, width), jnp.float32)
    two = jnp.zeros((1, width), jnp.float32)
    number = jnp.zeros((1, width), jnp.float32)
    for k in range(images):
        keep = (lax.broadcasted_iota(jnp.int32, (slots, 1), 0) < lens[k]).astype(jnp.float32)
        x = pix[k].astype(jnp.float32)
        kept = x * keep
        one = one + jnp.sum(kept, axis=0, keepdims=True)
        two = two + jnp.sum(kept * x, axis=0, keepdims=True)
        number = number + jnp.sum(keep, axis=0, keepdims=True)
    mine[...] = jnp.concatenate([one, two, number, jnp.zeros((5, width), jnp.float32)], axis=0)
    pl.semaphore_wait(bar, ranks - 1)

    def copy(k):
        peer = lax.rem(me + k, ranks)
        return pltpu.make_async_remote_copy(
            src_ref=mine, dst_ref=table.at[me], send_sem=ssem.at[k - 1], recv_sem=rsem.at[me],
            device_id=(peer, t), device_id_type=MESH)

    def arrival(k):
        peer = lax.rem(me + k, ranks)
        return pltpu.make_async_remote_copy(
            src_ref=mine, dst_ref=table.at[peer], send_sem=ssem.at[k - 1], recv_sem=rsem.at[peer],
            device_id=(peer, t), device_id_type=MESH)

    for k in range(1, ranks):
        copy(k).start()
    table[me] = mine[...]
    for k in range(1, ranks):
        arrival(k).wait_recv()
    total = table[0]
    for k in range(1, ranks):
        total = total + table[k]
    for k in range(1, ranks):
        copy(k).wait_send()
    for b in range(width // band_width):
        cols = slice(b * band_width, (b + 1) * band_width)
        count = total[2:3, cols] * float(band_width)
        mean = jnp.sum(total[0:1, cols], axis=1, keepdims=True) / count
        square = jnp.sum(total[1:2, cols], axis=1, keepdims=True) / count
        rstd = lax.rsqrt(square - mean * mean + 1e-05)
        out[:, cols] = jnp.concatenate(
            [mean, rstd, count, jnp.zeros((5, band_width), jnp.float32)], axis=0)


def band_stats(pixels, lengths, ranks):
    width = pixels.shape[2]
    return pl.pallas_call(
        functools.partial(stats_kernel, ranks, width // 3),
        out_shape=jax.ShapeDtypeStruct((8, width), jnp.float32),
        in_specs=[pl.BlockSpec(memory_space=pltpu.SMEM), pl.BlockSpec(memory_space=pltpu.VMEM)],
        out_specs=pl.BlockSpec(memory_space=pltpu.VMEM),
        scratch_shapes=[
            pltpu.VMEM((8, width), jnp.float32),
            pltpu.VMEM((ranks, 8, width), jnp.float32),
            pltpu.SemaphoreType.DMA((ranks,)),
            pltpu.SemaphoreType.DMA((ranks,)),
        ],
        compiler_params=pltpu.CompilerParams(collective_id=2, has_side_effects=True),
        name="band_stats")(lengths, pixels)


def positions(patch_ids, gsd_values, model_width, grid_side):
    quarter = model_width // 4
    gsd_scale = gsd_values.astype(jnp.float32) / 100.0
    row_pos = (patch_ids // grid_side).astype(jnp.float32) * gsd_scale[:, None]
    col_pos = (patch_ids % grid_side).astype(jnp.float32) * gsd_scale[:, None]
    frequency = jnp.exp(jnp.arange(quarter, dtype=jnp.float32) * (-math.log(10000.0) / quarter))
    row_angle = row_pos[:, :, None] * frequency
    col_angle = col_pos[:, :, None] * frequency
    return jnp.concatenate(
        [jnp.sin(row_angle), jnp.cos(row_angle), jnp.sin(col_angle), jnp.cos(col_angle)], axis=-1
    )


def contract_rows(left_side, right_side):
    return lax.dot_general(
        left_side, right_side, (((0,), (0,)), ((), ())), preferred_element_type=jnp.float32
    )


def contract_cols(left_side, right_side):
    return lax.dot_general(
        left_side, right_side, (((1,), (1,)), ((), ())), preferred_element_type=jnp.float32
    )


def normalize(hidden, gain_row, shift_row):
    centred = hidden - jnp.mean(hidden, axis=-1, keepdims=True)
    inverse = lax.rsqrt(jnp.mean(centred * centred, axis=-1, keepdims=True) + 1e-06)
    normed = centred * inverse
    return (normed * gain_row + shift_row, normed, inverse)


def normalize_back(upstream, normed, inverse, gain_row):
    scaled = upstream * gain_row
    return inverse * (
        scaled
        - jnp.mean(scaled, axis=-1, keepdims=True)
        - normed * jnp.mean(scaled * normed, axis=-1, keepdims=True)
    )


def gelu_slope(inputs):
    return 0.5 * (1.0 + lax.erf(inputs * (1.0 / math.sqrt(2.0)))) + inputs * jnp.exp(
        -0.5 * inputs * inputs
    ) * (1.0 / math.sqrt(2.0 * math.pi))


def tensor_sum(part):
    if lax.axis_size("tensor") != 2:
        return lax.psum(part, "tensor")
    return part + lax.ppermute(part, "tensor", [(0, 1), (1, 0)])


def per_device(
    fast,
    pixels,
    lengths,
    patch_ids,
    gsd_values,
    embed_w,
    embed_bias,
    norm_gain,
    norm_bias,
    qkv_w,
    qv_bias,
    out_w,
    out_bias,
    up_w,
    up_bias,
    down_w,
    down_bias,
    cotangent,
):
    images, slot_count, patch_width = pixels.shape
    band_width = patch_width // 3
    model_width = embed_w.shape[1]
    local_width = qkv_w.shape[2]
    head_dim = HD
    heads_here = local_width // head_dim
    tokens = images * slot_count
    score_scale = 1.0 / math.sqrt(head_dim)
    key_keep = jnp.arange(slot_count)[None, :] < lengths[:, None]
    valid_rows = key_keep.astype(jnp.float32)
    pixel_grid = pixels.astype(jnp.float32).reshape(images, slot_count, 3, band_width)
    pixel_mask = valid_rows[:, :, None, None]
    if fast:
        stats = band_stats(pixels, lengths, 16)
        band_mean = stats[0].reshape(3, band_width)[:, 0]
        band_rstd = stats[1].reshape(3, band_width)[:, 0]
        band_count = stats[2, 0]
    else:
        total_one, total_two, band_count = lax.psum(
            (
                jnp.sum(pixel_grid * pixel_mask, axis=(0, 1, 3)),
                jnp.sum(pixel_grid * pixel_grid * pixel_mask, axis=(0, 1, 3)),
                jnp.sum(valid_rows) * band_width,
            ),
            "dp",
        )
        band_mean = total_one / band_count
        band_rstd = lax.rsqrt(total_two / band_count - band_mean * band_mean + 1e-05)
    pixel_hat = (pixel_grid - band_mean[:, None]) * band_rstd[:, None]
    pixel_low = pixel_hat.reshape(tokens, patch_width).astype(jnp.bfloat16)
    pos_table = positions(patch_ids, gsd_values, model_width, GRID).reshape(tokens, model_width)
    stream_zero = (
        jnp.dot(pixel_low, embed_w, preferred_element_type=jnp.float32) + embed_bias + pos_table
    )
    layer_one, normed_one, inverse_one = normalize(stream_zero, norm_gain[0], norm_bias[0])
    attn_input = layer_one.astype(jnp.bfloat16)
    queries = (
        jnp.dot(attn_input, qkv_w[0], preferred_element_type=jnp.float32) + qv_bias[0]
    ).astype(jnp.bfloat16)
    key_rows = jnp.dot(attn_input, qkv_w[1], preferred_element_type=jnp.float32).astype(
        jnp.bfloat16
    )
    values = (
        jnp.dot(attn_input, qkv_w[2], preferred_element_type=jnp.float32) + qv_bias[1]
    ).astype(jnp.bfloat16)
    query_heads = queries.reshape(images, slot_count, heads_here, head_dim)
    key_heads = key_rows.reshape(images, slot_count, heads_here, head_dim)
    value_heads = values.reshape(images, slot_count, heads_here, head_dim)

    def score_block():
        scores = (
            jnp.einsum(
                "ichd,ijhd->ihcj", query_heads, key_heads, preferred_element_type=jnp.float32
            )
            * score_scale
        )
        return jnp.where(key_keep[:, None, None, :], scores, -1e30)

    scores = score_block()
    top_score = jnp.max(scores, axis=-1, keepdims=True)
    exp_scores = jnp.exp(scores - top_score)
    exp_total = jnp.sum(exp_scores, axis=-1, keepdims=True)
    log_total = top_score + jnp.log(exp_total)
    prob_low = (exp_scores / exp_total).astype(jnp.bfloat16)
    attended = (
        jnp.einsum("ihcj,ijhd->ichd", prob_low, value_heads, preferred_element_type=jnp.float32)
        .astype(jnp.bfloat16)
        .reshape(tokens, local_width)
    )
    attn_out = tensor_sum(jnp.dot(attended, out_w, preferred_element_type=jnp.float32))
    stream_one = stream_zero + attn_out + out_bias
    layer_two, normed_two, inverse_two = normalize(stream_one, norm_gain[1], norm_bias[1])
    mlp_input = layer_two.astype(jnp.bfloat16)
    hidden_pre = jnp.dot(mlp_input, up_w, preferred_element_type=jnp.float32) + up_bias
    hidden_low = jax.nn.gelu(hidden_pre, approximate=False).astype(jnp.bfloat16)
    mlp_part = jnp.dot(hidden_low, down_w, preferred_element_type=jnp.float32)
    row_valid = valid_rows.reshape(tokens, 1)
    grad_two = cotangent.astype(jnp.float32).reshape(tokens, model_width) * row_valid
    grad_down_bias = jnp.sum(grad_two, axis=0)
    grad_two_low = grad_two.astype(jnp.bfloat16)
    grad_down = contract_rows(hidden_low, grad_two_low)
    grad_hidden = (contract_cols(grad_two_low, down_w) * gelu_slope(hidden_pre)).astype(
        jnp.bfloat16
    )
    grad_up = contract_rows(mlp_input, grad_hidden)
    grad_up_bias = jnp.sum(grad_hidden.astype(jnp.float32), axis=0)
    grad_mlp_in = tensor_sum(contract_cols(grad_hidden, up_w))
    grad_one = grad_two + normalize_back(grad_mlp_in, normed_two, inverse_two, norm_gain[1])
    grad_out_bias = jnp.sum(grad_one, axis=0)
    grad_one_low = grad_one.astype(jnp.bfloat16)
    grad_out_proj = contract_rows(attended, grad_one_low)
    grad_attended = (
        contract_cols(grad_one_low, out_w)
        .astype(jnp.bfloat16)
        .reshape(images, slot_count, heads_here, head_dim)
    )
    attn_probs = jnp.exp(score_block() - log_total)
    grad_probs = jnp.einsum(
        "ichd,ijhd->ihcj", grad_attended, value_heads, preferred_element_type=jnp.float32
    )
    grad_values = jnp.einsum(
        "ihcj,ichd->ijhd",
        attn_probs.astype(jnp.bfloat16),
        grad_attended,
        preferred_element_type=jnp.float32,
    ).astype(jnp.bfloat16)
    prob_dot = jnp.sum(attn_probs * grad_probs, axis=-1, keepdims=True)
    grad_scores = (attn_probs * (grad_probs - prob_dot)).astype(jnp.bfloat16)
    grad_queries = (
        jnp.einsum("ihcj,ijhd->ichd", grad_scores, key_heads, preferred_element_type=jnp.float32)
        * score_scale
    ).astype(jnp.bfloat16)
    grad_keys = (
        jnp.einsum("ihcj,ichd->ijhd", grad_scores, query_heads, preferred_element_type=jnp.float32)
        * score_scale
    ).astype(jnp.bfloat16)
    grad_proj = (
        grad_queries.reshape(tokens, local_width),
        grad_keys.reshape(tokens, local_width),
        grad_values.reshape(tokens, local_width),
    )
    grad_qkv = jnp.stack([contract_rows(attn_input, grad_piece) for grad_piece in grad_proj])
    grad_qv_bias = jnp.stack(
        [
            jnp.sum(grad_proj[0].astype(jnp.float32), axis=0),
            jnp.sum(grad_proj[2].astype(jnp.float32), axis=0),
        ]
    )
    attn_partial = (
        contract_cols(grad_proj[0], qkv_w[0])
        + contract_cols(grad_proj[1], qkv_w[1])
        + contract_cols(grad_proj[2], qkv_w[2])
    )
    grad_attn_in = tensor_sum(attn_partial)
    mlp_part, _ = lax.optimization_barrier((mlp_part, grad_attn_in))
    stream_two = stream_one + tensor_sum(mlp_part) + down_bias
    output = (stream_two * row_valid).astype(jnp.bfloat16).reshape(images, slot_count, model_width)
    grad_zero = grad_one + normalize_back(grad_attn_in, normed_one, inverse_one, norm_gain[0])
    grad_norm_gain = jnp.stack(
        [jnp.sum(grad_attn_in * normed_one, axis=0), jnp.sum(grad_mlp_in * normed_two, axis=0)]
    )
    grad_norm_bias = jnp.stack([jnp.sum(grad_attn_in, axis=0), jnp.sum(grad_mlp_in, axis=0)])
    grad_embed_bias = jnp.sum(grad_zero, axis=0)
    grad_zero_low = grad_zero.astype(jnp.bfloat16)
    embed_part = contract_rows(pixel_low, grad_zero_low)
    grad_pixel_hat = contract_cols(grad_zero_low, embed_w).reshape(
        images, slot_count, 3, band_width
    )
    band_grad = jnp.sum(grad_pixel_hat, axis=(0, 1, 3))
    band_cross = jnp.sum(grad_pixel_hat * pixel_hat, axis=(0, 1, 3))
    small = (
        grad_qv_bias,
        grad_out_bias,
        grad_up_bias,
        grad_down_bias,
        grad_norm_gain,
        grad_norm_bias,
        grad_embed_bias,
        band_grad,
        band_cross,
    )
    large = (grad_qkv.reshape(-1, local_width), grad_out_proj, grad_up, grad_down, embed_part)
    if fast:
        packed = jnp.concatenate([piece.reshape(-1) for piece in small])
        packed = jnp.pad(packed, (0, 128 * W - packed.shape[0])).reshape(128, W)
        *large, packed = dp_sum((*large, packed))
        flat, at, pieces = packed.reshape(-1), 0, []
        for piece in small:
            pieces.append(flat[at : at + piece.size].reshape(piece.shape))
            at += piece.size
        small = pieces
    else:
        large, small = lax.psum((large, small), "dp")
    sum_qkv, sum_out_proj, sum_up, sum_down, embed_sum = large
    sum_qkv = sum_qkv.reshape(grad_qkv.shape)
    (
        sum_qv_bias,
        sum_out_bias,
        sum_up_bias,
        sum_down_bias,
        sum_gain,
        sum_shift,
        sum_embed_bias,
        band_grad_sum,
        band_cross_sum,
    ) = small
    pixel_grad = band_rstd[:, None] * (
        grad_pixel_hat
        - pixel_mask * (band_grad_sum[:, None] + band_cross_sum[:, None] * pixel_hat) / band_count
    )
    pixel_grad = pixel_grad.reshape(images, slot_count, patch_width)
    return (
        output,
        pixel_grad,
        embed_sum,
        sum_embed_bias,
        sum_gain,
        sum_shift,
        sum_qkv,
        sum_qv_bias,
        sum_out_proj,
        sum_out_bias,
        sum_up,
        sum_up_bias,
        sum_down,
        sum_down_bias,
    )


def solution(mesh):
    fast = dict(mesh.shape) == {"dp": 16, "tensor": 2}
    in_specs = (
        P("dp", None, None),
        P("dp"),
        P("dp", None),
        P("dp"),
        P(),
        P(),
        P(),
        P(),
        P(None, None, "tensor"),
        P(None, "tensor"),
        P("tensor", None),
        P(),
        P(None, "tensor"),
        P("tensor"),
        P("tensor", None),
        P(),
        P("dp", None, None),
    )
    out_specs = (
        P("dp", None, None),
        P("dp", None, None),
        P(),
        P(),
        P(),
        P(),
        P(None, None, "tensor"),
        P(None, "tensor"),
        P("tensor", None),
        P(),
        P(None, "tensor"),
        P("tensor"),
        P("tensor", None),
        P(),
    )
    return jax.shard_map(
        functools.partial(per_device, fast), mesh=mesh, in_specs=in_specs, out_specs=out_specs, check_vma=False
    )
```

```python
import functools
import math

import jax
import jax.numpy as jnp
from jax import lax
from jax.experimental import pallas as pl
from jax.experimental.pallas import tpu as pltpu
from jax.sharding import PartitionSpec as P

HD = 64
GRID = 28
MESH = pl.DeviceIdType.MESH
W = 512


SEND = (
    "c","x","oa","ob","ja","jb","xb","ga","gb","na","fa","nb","fb","xg","cg")

FETCH = 17


def back_kernel(shapes, R, K, delays, *refs):
    n = len(shapes)
    (lens, up_in, down_in, part_in, mlp_in, pre_in), fetched = refs[:6], refs[6 : 6 + FETCH]
    outs = refs[6 + FETCH : 6 + FETCH + n]
    mlp_out, pixel_out = refs[6 + FETCH + n : 8 + FETCH + n]
    scratch = refs[8 + FETCH + n :]
    held, scratch = scratch[:FETCH], scratch[FETCH:]
    (part, normed_two, inv_two, grad_two, attended, out_w, queries, keys, values, attn_in, qkv_w,
     normed_one, inv_one, pixel_low, pixel_hat, embed_w, gains) = held
    (land, land_two, back_part, grad_one, one_low, zero_low, grad_att, grad_proj, grad_pix, sums,
     out_grad, qkv_grad, embed_grad, small_grad) = scratch[:14]
    own, cl, xl, ab, oa, ob, ja, jb, nbuf, xbl, fin, ssem, rsem, lsem, fsem, ysend, yrecv = scratch[14:]
    ins = (up_in, down_in, out_grad, qkv_grad, embed_grad, small_grad)
    slots = normed_one.shape[0] // 2
    H, Q, E = R//2, R//4, R//8
    i = lax.axis_index("dp"); t = lax.axis_index("tensor")
    c = lax.rem(i, 2); x = lax.rem(i//2, 2); z = i//4
    side = z//2
    pos = lax.rem(z, 2)
    inner = lax.rem(side + pos, 2) == 1
    outer = lax.rem(side + pos, 2) == 0
    dev_c = (z*4 + x*2 + 1 - c, t)
    dev_x = (z*4 + (1-x)*2 + c, t)
    dev_o = ((side*2 + 1 - pos)*4 + x*2 + c, t)
    dev_j = ((3 - z)*4 + x*2 + c, t)
    dev_y = (i, 1 - t)
    fetches = [pltpu.make_async_copy(fetched[q], held[q], fsem.at[q]) for q in range(FETCH)]
    fetches.append(pltpu.make_async_copy(pre_in, small_grad.at[pl.ds(0, 8)], fsem.at[FETCH]))
    for q in fetches:
        q.start()
    bar = pltpu.get_barrier_semaphore()
    for d in (dev_c, dev_x, dev_o, dev_y):
        pl.semaphore_signal(bar, inc=1, device_id=d, device_id_type=MESH)
    @pl.when(inner)
    def _():
        pl.semaphore_signal(bar, inc=1, device_id=dev_j, device_id_type=MESH)
        pl.semaphore_wait(bar, 5)
    @pl.when(outer)
    def _():
        pl.semaphore_wait(bar, 4)
    def al(v, m): return pl.multiple_of(v, m)

    def across(q, src, dst):
        return pltpu.make_async_remote_copy(
            src_ref=src, dst_ref=dst, send_sem=ysend.at[q], recv_sem=yrecv.at[q],
            device_id=dev_y, device_id_type=MESH)

    first_sum = across(0, part_in, land)
    second_sum = across(1, back_part, land_two)
    third_sum = across(2, mlp_in, mlp_out)
    pixel_copy = pltpu.make_async_copy(grad_pix, pixel_out, fsem.at[FETCH + 1])
    first_sum.start()
    sums[...] = jnp.zeros_like(sums)
    small_grad[pl.ds(8, 120), :] = jnp.zeros((120, W), jnp.float32)
    f32, bf16 = jnp.float32, jnp.bfloat16

    def mm(a, b, ca, cb):
        return lax.dot_general(a, b, (((ca,), (cb,)), ((), ())), preferred_element_type=f32)

    def add_sum(row, value):
        width = value.shape[1]
        sums[row : row + 1, :width] = sums[row : row + 1, :width] + jnp.sum(value, axis=0, keepdims=True)

    def norm_back(upstream, normed, inverse, gain_row):
        scaled = upstream * gain_row
        return inverse * (
            scaled
            - jnp.mean(scaled, axis=-1, keepdims=True)
            - normed * jnp.mean(scaled * normed, axis=-1, keepdims=True))

    def second_norm(q):
        rows = pl.ds(al(q * 64, 64), 64)
        upstream, normed = part[rows, :] + land[rows, :], normed_two[rows, :]
        grad = grad_two[rows, :] + norm_back(upstream, normed, inv_two[rows, 0:1], gains[1:2, :])
        grad_one[rows, :] = grad
        one_low[rows, :] = grad.astype(bf16)
        add_sum(0, grad)
        add_sum(1, upstream * normed)
        add_sum(2, upstream)

    def into_heads(q):
        rows = pl.ds(al(q * 128, 128), 128)
        grad_att[rows, :] = mm(one_low[rows, :], out_w[...], 1, 1).astype(bf16)

    def attention(q):
        image, pair = q // 4, lax.rem(q, 4)
        rows, cols = pl.ds(al(image * slots, slots), slots), pl.ds(al(pair * 128, 128), 128)
        qs, ks, vs, gs = queries[rows, cols], keys[rows, cols], values[rows, cols], grad_att[rows, cols]
        keep = lax.broadcasted_iota(jnp.int32, (1, slots), 1) < lens[image]
        scale = 1.0 / math.sqrt(HD)
        dq, dk, dv = [], [], []
        for h in range(2):
            part_of = slice(h * HD, (h + 1) * HD)
            qh, kh, vh, gh = qs[:, part_of], ks[:, part_of], vs[:, part_of], gs[:, part_of]
            scores = jnp.where(keep, mm(qh, kh, 1, 1) * scale, -1e30)
            exps = jnp.exp(scores - jnp.max(scores, axis=-1, keepdims=True))
            probs = exps / jnp.sum(exps, axis=-1, keepdims=True)
            grad_probs = mm(gh, vh, 1, 1)
            dv.append(mm(probs.astype(bf16), gh, 0, 0))
            dot = jnp.sum(probs * grad_probs, axis=-1, keepdims=True)
            grad_scores = (probs * (grad_probs - dot)).astype(bf16)
            dq.append(mm(grad_scores, kh, 1, 0) * scale)
            dk.append(mm(grad_scores, qh, 0, 0) * scale)
        for at, pieces in enumerate((dq, dk, dv)):
            grad_proj[at, rows, cols] = jnp.concatenate(pieces, axis=1).astype(bf16)

    def into_norm(q):
        rows = pl.ds(al(q * 128, 128), 128)
        back_part[rows, :] = (
            mm(grad_proj[0, rows, :], qkv_w[0], 1, 1)
            + mm(grad_proj[1, rows, :], qkv_w[1], 1, 1)
            + mm(grad_proj[2, rows, :], qkv_w[2], 1, 1))

    def out_weight(q):
        cols = pl.ds(al(q * 128, 128), 128)
        out_grad[cols, :] = mm(attended[:, cols], one_low[...], 0, 0)

    def proj_weight(q):
        which, block = q // 4, lax.rem(q, 4)
        cols = pl.ds(al(block * 256, 256), 256)
        qkv_grad[pl.ds(al(q * 256, 256), 256), :] = mm(attn_in[:, cols], grad_proj[which], 0, 0)

    def first_norm(q):
        rows = pl.ds(al(q * 64, 64), 64)
        upstream, normed = back_part[rows, :] + land_two[rows, :], normed_one[rows, :]
        grad = grad_one[rows, :] + norm_back(upstream, normed, inv_one[rows, 0:1], gains[0:1, :])
        zero_low[rows, :] = grad.astype(bf16)
        add_sum(3, upstream * normed)
        add_sum(4, upstream)
        add_sum(5, grad)

    def embed_weight(q):
        cols = pl.ds(al(q * 256, 256), 256)
        embed_grad[cols, :] = mm(pixel_low[:, cols], zero_low[...], 0, 0)

    def pixels_back(q):
        rows = pl.ds(al(q * 128, 128), 128)
        grad = mm(zero_low[rows, :], embed_w[...], 1, 1)
        grad_pix[rows, :] = grad
        add_sum(6, grad)
        add_sum(7, grad * pixel_hat[rows, :])

    def pack(q):
        for row in range(8):
            small_grad[8 + 2 * row : 9 + 2 * row, :] = sums[row : row + 1, :W]
            small_grad[9 + 2 * row : 10 + 2 * row, :] = sums[row : row + 1, W:]
        for row, at in ((24, 0), (25, 2)):
            small_grad[row : row + 1, :] = jnp.sum(grad_proj[at].astype(f32), axis=0, keepdims=True)

    def fetch_wait(q):
        for one in fetches:
            one.wait()

    def first_wait(q):
        first_sum.wait()

    def second_start(q):
        second_sum.start()

    def second_wait(q):
        second_sum.wait()
        third_sum.start()

    def pixel_start(q):
        pixel_copy.start()

    plan = (
        (12, 1, fetch_wait), (23, 1, first_wait), (24, 8, second_norm), (32, 4, into_heads),
        (36, 8, attention), (44, 4, into_norm), (48, 1, second_start), (49, 4, out_weight),
        (53, 12, proj_weight), (71, 1, second_wait), (72, 8, first_norm), (80, 3, embed_weight),
        (83, 4, pixels_back), (87, 1, pack), (88, 1, pixel_start))
    starts, total = [], 0
    for (rows, cols) in shapes:
        starts.append(total); total += (rows//(2*R))*(cols//W)
    NC = total
    def slot(j): return lax.rem(j, K)
    a_mine = al(x*Q, Q); a_other = al((1-x)*Q, Q)
    e_near = al(side*E, E); e_far = al((1-side)*E, E)
    b_near = al(H + side*Q, Q); b_far = al(H + (1-side)*Q, Q)
    aN = al(x*Q + side*E, E); aF = al(x*Q + (1-side)*E, E)
    def hbm(ref, a, j, half):
        cols = shapes[a][1]//W
        q = j - starts[a]
        r = al((q//cols)*(2*R) + half*R, R)
        col = al(lax.rem(q, cols)*W, W)
        return ref.at[pl.ds(r, R), pl.ds(col, W)]
    def rc(kind, src, dst, dev, s):
        k = SEND.index(kind)
        return pltpu.make_async_remote_copy(src_ref=src, dst_ref=dst, send_sem=ssem.at[k, s], recv_sem=rsem.at[k, s], device_id=dev, device_id_type=MESH)
    def desc(kind, j):
        s = slot(j)
        if kind == "x": return rc(kind, own.at[s, pl.ds(a_other, Q)], xl.at[s], dev_x, s)
        if kind == "ob": return rc(kind, own.at[s, pl.ds(H, H)], ob.at[s], dev_o, s)
        if kind == "oa": return rc(kind, ab.at[s], oa.at[s], dev_o, s)
        if kind == "ja": return rc(kind, ab.at[s, pl.ds(e_far, E)], ja.at[s], dev_j, s)
        if kind == "jb": return rc(kind, own.at[s, pl.ds(b_far, Q)], jb.at[s], dev_j, s)
        if kind == "xb": return rc(kind, nbuf.at[s], xbl.at[s], dev_x, s)
        if kind in ("ga", "na"):
            return rc(kind, fin.at[s, pl.ds(aN, E)], fin.at[s, pl.ds(aN, E)], dev_j if kind == "ga" else dev_o, s)
        if kind == "fa": return rc(kind, fin.at[s, pl.ds(aF, E)], fin.at[s, pl.ds(aF, E)], dev_o, s)
        if kind in ("gb", "nb"):
            return rc(kind, fin.at[s, pl.ds(b_near, Q)], fin.at[s, pl.ds(b_near, Q)], dev_j if kind == "gb" else dev_o, s)
        if kind == "fb": return rc(kind, fin.at[s, pl.ds(b_far, Q)], fin.at[s, pl.ds(b_far, Q)], dev_o, s)
        if kind == "xg": return rc(kind, fin.at[s, pl.ds(a_mine, Q)], fin.at[s, pl.ds(a_mine, Q)], dev_x, s)
        if kind == "c": return rc(kind, hbm(ins[0], 0, starts[0], 1 - c), cl.at[s], dev_c, s)
        if kind == "cg": return rc(kind, fin.at[s], hbm(outs[0], 0, starts[0], c), dev_c, s)
        raise ValueError(kind)
    def each(j, f):
        for a in range(n):
            end = starts[a+1] if a + 1 < n else NC
            if n == 1: f(a); continue
            cond = (j >= starts[a]) & (j < end)
            pl.when(cond)(functools.partial(f, a))
    d = delays
    def step(tt, carry):
        js = [tt - dd for dd in d]
        def on(k): return (js[k] >= 0) & (js[k] < NC)
        @pl.when(on(7))
        def _():
            j = js[7]; s = slot(j)
            pltpu.make_async_copy(fin.at[s], hbm(outs[0], 0, starts[0], c), lsem.at[1, s]).wait()
            desc("cg", j).wait_send(); desc("cg", j).wait_recv()
            desc("c", j).wait_send(); desc("x", j).wait_send(); desc("xg", j).wait_send()
            @pl.when(outer)
            def _():
                desc("oa", j).wait_send(); desc("ob", j).wait_send()
            @pl.when(inner)
            def _():
                for k in ("ja","jb","xb","ga","gb","na","fa","nb","fb"): desc(k, j).wait_send()
        @pl.when(on(6))
        def _():
            j = js[6]
            desc("xg", j).wait_recv()
            @pl.when(outer)
            def _():
                desc("nb", j).wait_recv(); desc("fb", j).wait_recv()
        @pl.when(on(5))
        def _():
            j = js[5]
            @pl.when(inner)
            def _():
                desc("ga", j).wait_recv(); desc("gb", j).wait_recv()
        j5o = tt - d[5] - d[8]
        on5o = (j5o >= 0) & (j5o < NC)
        @pl.when(on5o & outer)
        def _():
            desc("na", j5o).wait_recv(); desc("fa", j5o).wait_recv()
        @pl.when(on(4))
        def _():
            j = js[4]; s = slot(j)
            @pl.when(inner)
            def _():
                desc("ja", j).wait_recv(); desc("xb", j).wait_recv()
                fin[s, pl.ds(aN, E)] = ab[s, pl.ds(e_near, E)] + ja[s]
                fin[s, pl.ds(b_near, Q)] = nbuf[s] + xbl[s]
        @pl.when(on(3))
        def _():
            j = js[3]; s = slot(j)
            @pl.when(inner)
            def _():
                desc("oa", j).wait_recv(); desc("jb", j).wait_recv()
                ab[s] = ab[s] + oa[s]
                nbuf[s] = own[s, pl.ds(b_near, Q)] + jb[s]
        @pl.when(on(2))
        def _():
            j = js[2]; s = slot(j)
            desc("x", j).wait_recv()
            ab[s] = own[s, pl.ds(a_mine, Q)] + xl[s]
            @pl.when(inner)
            def _():
                desc("ob", j).wait_recv()
                own[s, pl.ds(H, H)] = own[s, pl.ds(H, H)] + ob[s]
        @pl.when(on(1))
        def _():
            j = js[1]; s = slot(j)
            pltpu.make_async_copy(hbm(ins[0], 0, starts[0], c), own.at[s], lsem.at[0, s]).wait()
            desc("c", j).wait_recv()
            own[s] = own[s] + cl[s]
        @pl.when(on(6))
        def _():
            j = js[6]; s = slot(j)
            def f(a):
                pltpu.make_async_copy(fin.at[s], hbm(outs[a], a, j, c), lsem.at[1, s]).start()
                rc("cg", fin.at[s], hbm(outs[a], a, j, c), dev_c, s).start()
            each(j, f)
        @pl.when(on(5))
        def _():
            j = js[5]
            @pl.when(inner)
            def _():
                desc("fa", j).start(); desc("xg", j).start(); desc("fb", j).start()
        @pl.when(on5o & outer)
        def _():
            desc("xg", j5o).start()
        @pl.when(on(4))
        def _():
            j = js[4]
            @pl.when(inner)
            def _():
                for k in ("ga","na","gb","nb"): desc(k, j).start()
        @pl.when(on(3))
        def _():
            j = js[3]
            @pl.when(inner)
            def _():
                desc("ja", j).start(); desc("xb", j).start()
        @pl.when(on(2))
        def _():
            j = js[2]
            @pl.when(outer)
            def _(): desc("oa", j).start()
            @pl.when(inner)
            def _(): desc("jb", j).start()
        @pl.when(on(1))
        def _():
            j = js[1]
            desc("x", j).start()
            @pl.when(outer)
            def _(): desc("ob", j).start()
        @pl.when(on(0))
        def _():
            j = js[0]; s = slot(j)
            def f(a):
                pltpu.make_async_copy(hbm(ins[a], a, j, c), own.at[s], lsem.at[0, s]).start()
                rc("c", hbm(ins[a], a, j, 1 - c), cl.at[s], dev_c, s).start()
            each(j, f)
        for begin, number, piece in plan:
            if number == 1:
                pl.when(tt == begin)(functools.partial(piece, 0))
            else:
                pl.when((tt >= begin) & (tt < begin + number))(functools.partial(piece, tt - begin))
        return carry
    lax.fori_loop(0, NC + d[7], step, 0)
    third_sum.wait()
    pixel_copy.wait()


def back_pass(lengths, grad_up, grad_down, part, mlp_part, pre, fetched, R=64, K=14,
              delays=(0, 1, 3, 5, 7, 9, 12, 13, 1)):
    f32, bf16 = jnp.float32, jnp.bfloat16
    tokens, width = part.shape
    local = grad_up.shape[0] // 2
    patch = fetched[13].shape[1]
    shapes = (grad_up.shape, grad_down.shape, (local, width), (3 * width, local), (patch, width), (2 * R, W))
    n = len(shapes)
    H, Q, E = R // 2, R // 4, R // 8
    V = lambda r: pltpu.VMEM((K, r, W), f32)
    anywhere = pl.BlockSpec(memory_space=pl.ANY)
    held = [pltpu.VMEM(a.shape, a.dtype) for a in fetched]
    out = [jax.ShapeDtypeStruct(s, f32) for s in shapes]
    out += [jax.ShapeDtypeStruct((tokens, width), f32), jax.ShapeDtypeStruct((tokens, patch), f32)]
    return pl.pallas_call(
        functools.partial(back_kernel, shapes, R, K, delays),
        out_shape=out,
        in_specs=[pl.BlockSpec(memory_space=pltpu.SMEM)] + [anywhere] * (5 + FETCH),
        out_specs=[anywhere] * len(out),
        scratch_shapes=[
            *held,
            pltpu.VMEM((tokens, width), f32), pltpu.VMEM((tokens, width), f32), pltpu.VMEM((tokens, width), f32),
            pltpu.VMEM((tokens, width), f32), pltpu.VMEM((tokens, width), bf16), pltpu.VMEM((tokens, width), bf16),
            pltpu.VMEM((tokens, local), bf16), pltpu.VMEM((3, tokens, local), bf16),
            pltpu.VMEM((tokens, patch), f32), pltpu.VMEM((8, width), f32),
            pltpu.VMEM(shapes[2], f32), pltpu.VMEM(shapes[3], f32), pltpu.VMEM(shapes[4], f32), pltpu.VMEM(shapes[5], f32),
            V(R), V(R), V(Q), V(Q), V(Q), V(H), V(E), V(Q), V(Q), V(Q), V(R),
            pltpu.SemaphoreType.DMA((len(SEND), K)), pltpu.SemaphoreType.DMA((len(SEND), K)),
            pltpu.SemaphoreType.DMA((2, K)), pltpu.SemaphoreType.DMA((FETCH + 2,)),
            pltpu.SemaphoreType.DMA((3,)), pltpu.SemaphoreType.DMA((3,)),
        ],
        compiler_params=pltpu.CompilerParams(collective_id=1, has_side_effects=True, vmem_limit_bytes=66_000_000),
        name="back_pass")(lengths, grad_up, grad_down, part, mlp_part, pre, *fetched)


def stats_kernel(ranks, band_width, lens, pix, out, mine, table, ssem, rsem):
    me = lax.axis_index("dp")
    t = lax.axis_index("tensor")
    bar = pltpu.get_barrier_semaphore()
    for k in range(1, ranks):
        pl.semaphore_signal(bar, inc=1, device_id=(lax.rem(me + k, ranks), t), device_id_type=MESH)
    images, slots, width = pix.shape
    one = jnp.zeros((1, width), jnp.float32)
    two = jnp.zeros((1, width), jnp.float32)
    number = jnp.zeros((1, width), jnp.float32)
    for k in range(images):
        keep = (lax.broadcasted_iota(jnp.int32, (slots, 1), 0) < lens[k]).astype(jnp.float32)
        x = pix[k].astype(jnp.float32)
        kept = x * keep
        one = one + jnp.sum(kept, axis=0, keepdims=True)
        two = two + jnp.sum(kept * x, axis=0, keepdims=True)
        number = number + jnp.sum(keep, axis=0, keepdims=True)
    mine[...] = jnp.concatenate([one, two, number, jnp.zeros((5, width), jnp.float32)], axis=0)
    pl.semaphore_wait(bar, ranks - 1)

    def copy(k):
        peer = lax.rem(me + k, ranks)
        return pltpu.make_async_remote_copy(
            src_ref=mine, dst_ref=table.at[me], send_sem=ssem.at[k - 1], recv_sem=rsem.at[me],
            device_id=(peer, t), device_id_type=MESH)

    def arrival(k):
        peer = lax.rem(me + k, ranks)
        return pltpu.make_async_remote_copy(
            src_ref=mine, dst_ref=table.at[peer], send_sem=ssem.at[k - 1], recv_sem=rsem.at[peer],
            device_id=(peer, t), device_id_type=MESH)

    for k in range(1, ranks):
        copy(k).start()
    table[me] = mine[...]
    for k in range(1, ranks):
        arrival(k).wait_recv()
    total = table[0]
    for k in range(1, ranks):
        total = total + table[k]
    for k in range(1, ranks):
        copy(k).wait_send()
    for b in range(width // band_width):
        cols = slice(b * band_width, (b + 1) * band_width)
        count = total[2:3, cols] * float(band_width)
        mean = jnp.sum(total[0:1, cols], axis=1, keepdims=True) / count
        square = jnp.sum(total[1:2, cols], axis=1, keepdims=True) / count
        rstd = lax.rsqrt(square - mean * mean + 1e-05)
        out[:, cols] = jnp.concatenate(
            [mean, rstd, count, jnp.zeros((5, band_width), jnp.float32)], axis=0)


def band_stats(pixels, lengths, ranks):
    width = pixels.shape[2]
    return pl.pallas_call(
        functools.partial(stats_kernel, ranks, width // 3),
        out_shape=jax.ShapeDtypeStruct((8, width), jnp.float32),
        in_specs=[pl.BlockSpec(memory_space=pltpu.SMEM), pl.BlockSpec(memory_space=pltpu.VMEM)],
        out_specs=pl.BlockSpec(memory_space=pltpu.VMEM),
        scratch_shapes=[
            pltpu.VMEM((8, width), jnp.float32),
            pltpu.VMEM((ranks, 8, width), jnp.float32),
            pltpu.SemaphoreType.DMA((ranks,)),
            pltpu.SemaphoreType.DMA((ranks,)),
        ],
        compiler_params=pltpu.CompilerParams(collective_id=2, has_side_effects=True),
        name="band_stats")(lengths, pixels)


def positions(patch_ids, gsd_values, model_width, grid_side):
    quarter = model_width // 4
    gsd_scale = gsd_values.astype(jnp.float32) / 100.0
    row_pos = (patch_ids // grid_side).astype(jnp.float32) * gsd_scale[:, None]
    col_pos = (patch_ids % grid_side).astype(jnp.float32) * gsd_scale[:, None]
    frequency = jnp.exp(jnp.arange(quarter, dtype=jnp.float32) * (-math.log(10000.0) / quarter))
    row_angle = row_pos[:, :, None] * frequency
    col_angle = col_pos[:, :, None] * frequency
    return jnp.concatenate(
        [jnp.sin(row_angle), jnp.cos(row_angle), jnp.sin(col_angle), jnp.cos(col_angle)], axis=-1
    )


def contract_rows(left_side, right_side):
    return lax.dot_general(
        left_side, right_side, (((0,), (0,)), ((), ())), preferred_element_type=jnp.float32
    )


def contract_cols(left_side, right_side):
    return lax.dot_general(
        left_side, right_side, (((1,), (1,)), ((), ())), preferred_element_type=jnp.float32
    )


def normalize(hidden, gain_row, shift_row):
    centred = hidden - jnp.mean(hidden, axis=-1, keepdims=True)
    inverse = lax.rsqrt(jnp.mean(centred * centred, axis=-1, keepdims=True) + 1e-06)
    normed = centred * inverse
    return (normed * gain_row + shift_row, normed, inverse)


def normalize_back(upstream, normed, inverse, gain_row):
    scaled = upstream * gain_row
    return inverse * (
        scaled
        - jnp.mean(scaled, axis=-1, keepdims=True)
        - normed * jnp.mean(scaled * normed, axis=-1, keepdims=True)
    )


def gelu_slope(inputs):
    return 0.5 * (1.0 + lax.erf(inputs * (1.0 / math.sqrt(2.0)))) + inputs * jnp.exp(
        -0.5 * inputs * inputs
    ) * (1.0 / math.sqrt(2.0 * math.pi))


def tensor_sum(part):
    if lax.axis_size("tensor") != 2:
        return lax.psum(part, "tensor")
    return part + lax.ppermute(part, "tensor", [(0, 1), (1, 0)])


def per_device(
    fast,
    pixels,
    lengths,
    patch_ids,
    gsd_values,
    embed_w,
    embed_bias,
    norm_gain,
    norm_bias,
    qkv_w,
    qv_bias,
    out_w,
    out_bias,
    up_w,
    up_bias,
    down_w,
    down_bias,
    cotangent,
):
    images, slot_count, patch_width = pixels.shape
    band_width = patch_width // 3
    model_width = embed_w.shape[1]
    local_width = qkv_w.shape[2]
    head_dim = HD
    heads_here = local_width // head_dim
    tokens = images * slot_count
    score_scale = 1.0 / math.sqrt(head_dim)
    key_keep = jnp.arange(slot_count)[None, :] < lengths[:, None]
    valid_rows = key_keep.astype(jnp.float32)
    pixel_grid = pixels.astype(jnp.float32).reshape(images, slot_count, 3, band_width)
    pixel_mask = valid_rows[:, :, None, None]
    if fast:
        stats = band_stats(pixels, lengths, 16)
        band_mean = stats[0].reshape(3, band_width)[:, 0]
        band_rstd = stats[1].reshape(3, band_width)[:, 0]
        band_count = stats[2, 0]
    else:
        total_one, total_two, band_count = lax.psum(
            (
                jnp.sum(pixel_grid * pixel_mask, axis=(0, 1, 3)),
                jnp.sum(pixel_grid * pixel_grid * pixel_mask, axis=(0, 1, 3)),
                jnp.sum(valid_rows) * band_width,
            ),
            "dp",
        )
        band_mean = total_one / band_count
        band_rstd = lax.rsqrt(total_two / band_count - band_mean * band_mean + 1e-05)
    pixel_hat = (pixel_grid - band_mean[:, None]) * band_rstd[:, None]
    pixel_low = pixel_hat.reshape(tokens, patch_width).astype(jnp.bfloat16)
    pos_table = positions(patch_ids, gsd_values, model_width, GRID).reshape(tokens, model_width)
    stream_zero = (
        jnp.dot(pixel_low, embed_w, preferred_element_type=jnp.float32) + embed_bias + pos_table
    )
    layer_one, normed_one, inverse_one = normalize(stream_zero, norm_gain[0], norm_bias[0])
    attn_input = layer_one.astype(jnp.bfloat16)
    queries = (
        jnp.dot(attn_input, qkv_w[0], preferred_element_type=jnp.float32) + qv_bias[0]
    ).astype(jnp.bfloat16)
    key_rows = jnp.dot(attn_input, qkv_w[1], preferred_element_type=jnp.float32).astype(
        jnp.bfloat16
    )
    values = (
        jnp.dot(attn_input, qkv_w[2], preferred_element_type=jnp.float32) + qv_bias[1]
    ).astype(jnp.bfloat16)
    query_heads = queries.reshape(images, slot_count, heads_here, head_dim)
    key_heads = key_rows.reshape(images, slot_count, heads_here, head_dim)
    value_heads = values.reshape(images, slot_count, heads_here, head_dim)

    def score_block():
        scores = (
            jnp.einsum(
                "ichd,ijhd->ihcj", query_heads, key_heads, preferred_element_type=jnp.float32
            )
            * score_scale
        )
        return jnp.where(key_keep[:, None, None, :], scores, -1e30)

    scores = score_block()
    top_score = jnp.max(scores, axis=-1, keepdims=True)
    exp_scores = jnp.exp(scores - top_score)
    exp_total = jnp.sum(exp_scores, axis=-1, keepdims=True)
    log_total = top_score + jnp.log(exp_total)
    prob_low = (exp_scores / exp_total).astype(jnp.bfloat16)
    attended = (
        jnp.einsum("ihcj,ijhd->ichd", prob_low, value_heads, preferred_element_type=jnp.float32)
        .astype(jnp.bfloat16)
        .reshape(tokens, local_width)
    )
    attn_out = tensor_sum(jnp.dot(attended, out_w, preferred_element_type=jnp.float32))
    stream_one = stream_zero + attn_out + out_bias
    layer_two, normed_two, inverse_two = normalize(stream_one, norm_gain[1], norm_bias[1])
    mlp_input = layer_two.astype(jnp.bfloat16)
    hidden_pre = jnp.dot(mlp_input, up_w, preferred_element_type=jnp.float32) + up_bias
    hidden_low = jax.nn.gelu(hidden_pre, approximate=False).astype(jnp.bfloat16)
    mlp_part = jnp.dot(hidden_low, down_w, preferred_element_type=jnp.float32)
    row_valid = valid_rows.reshape(tokens, 1)
    grad_two = cotangent.astype(jnp.float32).reshape(tokens, model_width) * row_valid
    grad_down_bias = jnp.sum(grad_two, axis=0)
    grad_two_low = grad_two.astype(jnp.bfloat16)
    grad_down = contract_rows(hidden_low, grad_two_low)
    grad_hidden = (contract_cols(grad_two_low, down_w) * gelu_slope(hidden_pre)).astype(
        jnp.bfloat16
    )
    grad_up = contract_rows(mlp_input, grad_hidden)
    grad_up_bias = jnp.sum(grad_hidden.astype(jnp.float32), axis=0)
    if fast:
        spread = lambda column: jnp.broadcast_to(column, (tokens, 128))
        pre = jnp.concatenate([grad_up_bias, jnp.sum(grad_two, axis=0), jnp.zeros((1024,), jnp.float32)])
        fetched = (
            contract_cols(grad_hidden, up_w), normed_two, spread(inverse_two), grad_two, attended, out_w,
            queries, key_rows, values, attn_input, qkv_w, normed_one, spread(inverse_one), pixel_low,
            pixel_hat.reshape(tokens, patch_width), embed_w, norm_gain)
        sum_up, sum_down, sum_out_proj, sum_qkv, embed_sum, small, mlp_other, grad_pixel_hat = back_pass(
            lengths, grad_up, grad_down, fetched[0], mlp_part, pre.reshape(8, W), fetched)
        flat = small.reshape(-1)
        rows = small[8:24].reshape(8, 2 * W)
        sum_up_bias, sum_down_bias = flat[:2048], flat[2048:3072]
        band = rows[6:8, :patch_width].reshape(2, 3, band_width).sum(axis=-1)
        stream_two = stream_one + (mlp_part + mlp_other) + down_bias
        output = (stream_two * row_valid).astype(jnp.bfloat16).reshape(images, slot_count, model_width)
        grad_pixel_hat = grad_pixel_hat.reshape(images, slot_count, 3, band_width)
        pixel_grad = band_rstd[:, None] * (
            grad_pixel_hat
            - pixel_mask * (band[0][:, None] + band[1][:, None] * pixel_hat) / band_count
        )
        return (
            output,
            pixel_grad.reshape(images, slot_count, patch_width),
            embed_sum,
            rows[5],
            jnp.stack([rows[3], rows[1]]),
            jnp.stack([rows[4], rows[2]]),
            sum_qkv.reshape(3, model_width, local_width),
            small[24:26],
            sum_out_proj,
            rows[0],
            sum_up,
            sum_up_bias,
            sum_down,
            sum_down_bias,
        )
    grad_mlp_in = tensor_sum(contract_cols(grad_hidden, up_w))
    grad_one = grad_two + normalize_back(grad_mlp_in, normed_two, inverse_two, norm_gain[1])
    grad_out_bias = jnp.sum(grad_one, axis=0)
    grad_one_low = grad_one.astype(jnp.bfloat16)
    grad_out_proj = contract_rows(attended, grad_one_low)
    grad_attended = (
        contract_cols(grad_one_low, out_w)
        .astype(jnp.bfloat16)
        .reshape(images, slot_count, heads_here, head_dim)
    )
    attn_probs = jnp.exp(score_block() - log_total)
    grad_probs = jnp.einsum(
        "ichd,ijhd->ihcj", grad_attended, value_heads, preferred_element_type=jnp.float32
    )
    grad_values = jnp.einsum(
        "ihcj,ichd->ijhd",
        attn_probs.astype(jnp.bfloat16),
        grad_attended,
        preferred_element_type=jnp.float32,
    ).astype(jnp.bfloat16)
    prob_dot = jnp.sum(attn_probs * grad_probs, axis=-1, keepdims=True)
    grad_scores = (attn_probs * (grad_probs - prob_dot)).astype(jnp.bfloat16)
    grad_queries = (
        jnp.einsum("ihcj,ijhd->ichd", grad_scores, key_heads, preferred_element_type=jnp.float32)
        * score_scale
    ).astype(jnp.bfloat16)
    grad_keys = (
        jnp.einsum("ihcj,ichd->ijhd", grad_scores, query_heads, preferred_element_type=jnp.float32)
        * score_scale
    ).astype(jnp.bfloat16)
    grad_proj = (
        grad_queries.reshape(tokens, local_width),
        grad_keys.reshape(tokens, local_width),
        grad_values.reshape(tokens, local_width),
    )
    grad_qkv = jnp.stack([contract_rows(attn_input, grad_piece) for grad_piece in grad_proj])
    grad_qv_bias = jnp.stack(
        [
            jnp.sum(grad_proj[0].astype(jnp.float32), axis=0),
            jnp.sum(grad_proj[2].astype(jnp.float32), axis=0),
        ]
    )
    attn_partial = (
        contract_cols(grad_proj[0], qkv_w[0])
        + contract_cols(grad_proj[1], qkv_w[1])
        + contract_cols(grad_proj[2], qkv_w[2])
    )
    grad_attn_in = tensor_sum(attn_partial)
    mlp_part, _ = lax.optimization_barrier((mlp_part, grad_attn_in))
    stream_two = stream_one + tensor_sum(mlp_part) + down_bias
    output = (stream_two * row_valid).astype(jnp.bfloat16).reshape(images, slot_count, model_width)
    grad_zero = grad_one + normalize_back(grad_attn_in, normed_one, inverse_one, norm_gain[0])
    grad_norm_gain = jnp.stack(
        [jnp.sum(grad_attn_in * normed_one, axis=0), jnp.sum(grad_mlp_in * normed_two, axis=0)]
    )
    grad_norm_bias = jnp.stack([jnp.sum(grad_attn_in, axis=0), jnp.sum(grad_mlp_in, axis=0)])
    grad_embed_bias = jnp.sum(grad_zero, axis=0)
    grad_zero_low = grad_zero.astype(jnp.bfloat16)
    embed_part = contract_rows(pixel_low, grad_zero_low)
    grad_pixel_hat = contract_cols(grad_zero_low, embed_w).reshape(
        images, slot_count, 3, band_width
    )
    band_grad = jnp.sum(grad_pixel_hat, axis=(0, 1, 3))
    band_cross = jnp.sum(grad_pixel_hat * pixel_hat, axis=(0, 1, 3))
    small = (
        grad_qv_bias,
        grad_out_bias,
        grad_up_bias,
        grad_down_bias,
        grad_norm_gain,
        grad_norm_bias,
        grad_embed_bias,
        band_grad,
        band_cross,
    )
    large = (grad_qkv.reshape(-1, local_width), grad_out_proj, grad_up, grad_down, embed_part)
    large, small = lax.psum((large, small), "dp")
    sum_qkv, sum_out_proj, sum_up, sum_down, embed_sum = large
    sum_qkv = sum_qkv.reshape(grad_qkv.shape)
    (
        sum_qv_bias,
        sum_out_bias,
        sum_up_bias,
        sum_down_bias,
        sum_gain,
        sum_shift,
        sum_embed_bias,
        band_grad_sum,
        band_cross_sum,
    ) = small
    pixel_grad = band_rstd[:, None] * (
        grad_pixel_hat
        - pixel_mask * (band_grad_sum[:, None] + band_cross_sum[:, None] * pixel_hat) / band_count
    )
    pixel_grad = pixel_grad.reshape(images, slot_count, patch_width)
    return (
        output,
        pixel_grad,
        embed_sum,
        sum_embed_bias,
        sum_gain,
        sum_shift,
        sum_qkv,
        sum_qv_bias,
        sum_out_proj,
        sum_out_bias,
        sum_up,
        sum_up_bias,
        sum_down,
        sum_down_bias,
    )


def solution(mesh):
    fast = dict(mesh.shape) == {"dp": 16, "tensor": 2}
    in_specs = (
        P("dp", None, None),
        P("dp"),
        P("dp", None),
        P("dp"),
        P(),
        P(),
        P(),
        P(),
        P(None, None, "tensor"),
        P(None, "tensor"),
        P("tensor", None),
        P(),
        P(None, "tensor"),
        P("tensor"),
        P("tensor", None),
        P(),
        P("dp", None, None),
    )
    out_specs = (
        P("dp", None, None),
        P("dp", None, None),
        P(),
        P(),
        P(),
        P(),
        P(None, None, "tensor"),
        P(None, "tensor"),
        P("tensor", None),
        P(),
        P(None, "tensor"),
        P("tensor"),
        P("tensor", None),
        P(),
    )
    return jax.shard_map(
        functools.partial(per_device, fast), mesh=mesh, in_specs=in_specs, out_specs=out_specs, check_vma=False
    )
```

```python
import functools
import math

import jax
import jax.numpy as jnp
from jax import lax
from jax.experimental import pallas as pl
from jax.experimental.pallas import tpu as pltpu
from jax.sharding import PartitionSpec as P

HD = 64
GRID = 28
MESH = pl.DeviceIdType.MESH
W = 512


SEND = (
    "c","x","oa","ob","ja","jb","xb","ga","gb","na","fa","nb","fb","xg","cg")

FETCH = 23


def back_kernel(shapes, R, K, delays, *refs):
    n = len(shapes)
    lens = refs[0]
    fetched = refs[1 : 1 + FETCH]
    outs = refs[1 + FETCH : 1 + FETCH + n]
    ins = refs[1 + FETCH + n : 1 + FETCH + 2 * n - 1]
    layer_out, pixel_out = refs[FETCH + 2 * n : FETCH + 2 * n + 2]
    scratch = refs[FETCH + 2 * n + 2 :]
    held, scratch = scratch[:FETCH], scratch[FETCH:]
    (mlp_in, up_w, down_w, up_bias, two_low, stream_one, mean_two, inv_two, attended, out_w, queries,
     keys, values, attn_in, qkv_w, normed_one, inv_one, pixel_low, pixel_hat, embed_w, gains, down_bias,
     stats) = held
    (part, mlp_part, land, land_two, grad_one, one_low, zero_low, grad_att, grad_proj, grad_pix, hidden,
     grad_hid, sums, up_sum, down_sum, small_grad, small_total, tall, wide) = scratch[:19]
    own, cl, xl, ab, oa, ob, ja, jb, nbuf, xbl, fin, ssem, rsem, lsem, fsem, wsem, ysend, yrecv = scratch[19:]
    ins = (*ins[:4], small_grad, ins[4])
    slots = normed_one.shape[0] // 2
    blocks = hidden.shape[1] // W
    H, Q, E = R//2, R//4, R//8
    i = lax.axis_index("dp"); t = lax.axis_index("tensor")
    c = lax.rem(i, 2); x = lax.rem(i//2, 2); z = i//4
    side = z//2
    pos = lax.rem(z, 2)
    inner = lax.rem(side + pos, 2) == 1
    outer = lax.rem(side + pos, 2) == 0
    dev_c = (z*4 + x*2 + 1 - c, t)
    dev_x = (z*4 + (1-x)*2 + c, t)
    dev_o = ((side*2 + 1 - pos)*4 + x*2 + c, t)
    dev_j = ((3 - z)*4 + x*2 + c, t)
    dev_y = (i, 1 - t)
    fetches = [pltpu.make_async_copy(fetched[q], held[q], fsem.at[q]) for q in range(FETCH)]
    for q in fetches:
        q.start()
    bar = pltpu.get_barrier_semaphore()
    for d in (dev_c, dev_x, dev_o, dev_y):
        pl.semaphore_signal(bar, inc=1, device_id=d, device_id_type=MESH)
    @pl.when(inner)
    def _():
        pl.semaphore_signal(bar, inc=1, device_id=dev_j, device_id_type=MESH)
        pl.semaphore_wait(bar, 5)
    @pl.when(outer)
    def _():
        pl.semaphore_wait(bar, 4)
    def al(v, m): return pl.multiple_of(v, m)

    def across(q, src, dst):
        return pltpu.make_async_remote_copy(
            src_ref=src, dst_ref=dst, send_sem=ysend.at[q], recv_sem=yrecv.at[q],
            device_id=dev_y, device_id_type=MESH)

    def image_rows(q):
        return pl.ds(q * slots, slots)

    first_sum = [across(q, part.at[image_rows(q)], land.at[image_rows(q)]) for q in range(2)]
    second_sum = [across(2 + q, part.at[image_rows(q)], land_two.at[image_rows(q)]) for q in range(2)]
    third_sum = across(4, mlp_part, land)
    pixel_copy = pltpu.make_async_copy(grad_pix, pixel_out, wsem.at[5])
    layer_copy = pltpu.make_async_copy(one_low, layer_out, wsem.at[6])
    total_copy = pltpu.make_async_copy(outs[4].at[pl.ds(0, 32)], small_total, wsem.at[7])
    sums[...] = jnp.zeros_like(sums)
    small_grad[...] = jnp.zeros_like(small_grad)
    up_sum[...] = jnp.zeros_like(up_sum)
    down_sum[...] = jnp.zeros_like(down_sum)
    f32, bf16 = jnp.float32, jnp.bfloat16

    def mm(a, b, ca, cb):
        return lax.dot_general(a, b, (((ca,), (cb,)), ((), ())), preferred_element_type=f32)

    def add_sum(row, value):
        width = value.shape[1]
        sums[row : row + 1, :width] = sums[row : row + 1, :width] + jnp.sum(value, axis=0, keepdims=True)

    def norm_back(upstream, normed, inverse, gain_row):
        scaled = upstream * gain_row
        return inverse * (
            scaled
            - jnp.mean(scaled, axis=-1, keepdims=True)
            - normed * jnp.mean(scaled * normed, axis=-1, keepdims=True))

    def feed(q):
        block, rows = q // 4, pl.ds(al(lax.rem(q, 4) * 128, 128), 128)
        cols = pl.ds(al(block * W, W), W)
        low = two_low[rows, :]
        up_block, down_block = up_w[:, cols], down_w[cols, :]
        u = mm(mlp_in[rows, :], up_block, 1, 0) + up_bias[0:1, cols]
        below = 0.5 * (1.0 + lax.erf(u * (1.0 / math.sqrt(2.0))))
        hid = (u * below).astype(bf16)
        slope = below + u * jnp.exp(-0.5 * u * u) * (1.0 / math.sqrt(2.0 * math.pi))
        grad = (mm(low, down_block, 1, 1) * slope).astype(bf16)
        hidden[rows, cols] = hid
        grad_hid[rows, cols] = grad
        up_sum[0:1, cols] = up_sum[0:1, cols] + jnp.sum(grad.astype(f32), axis=0, keepdims=True)
        to_in, to_out = mm(grad, up_block, 1, 1), mm(hid, down_block, 1, 0)

        @pl.when(block == 0)
        def _():
            part[rows, :] = to_in
            mlp_part[rows, :] = to_out

        @pl.when(block > 0)
        def _():
            part[rows, :] = part[rows, :] + to_in
            mlp_part[rows, :] = mlp_part[rows, :] + to_out

    def down_store(q):
        return pltpu.make_async_copy(tall, ins[1].at[pl.ds(al(q * 256, 256), 256)], wsem.at[0])

    def up_store(q):
        rows = pl.ds(al(lax.rem(q, 2) * 512, 512), 512)
        return pltpu.make_async_copy(wide, ins[0].at[rows, pl.ds(al((q // 2) * W, W), W)], wsem.at[1])

    def out_store(q):
        return pltpu.make_async_copy(
            tall.at[pl.ds(0, 128)], ins[2].at[pl.ds(al(q * 128, 128), 128)], wsem.at[2])

    def proj_store(q):
        return pltpu.make_async_copy(
            wide.at[pl.ds(0, 256)], ins[3].at[pl.ds(al(q * 256, 256), 256)], wsem.at[3])

    def embed_store(q):
        return pltpu.make_async_copy(tall, ins[5].at[pl.ds(al(q * 256, 256), 256)], wsem.at[4])

    def down_weight(q):
        tall[...] = mm(hidden[:, pl.ds(al(q * 256, 256), 256)], two_low[...], 0, 0)
        down_store(q).start()

    def up_weight(q):
        cols = pl.ds(al(lax.rem(q, 2) * 512, 512), 512)
        wide[...] = mm(mlp_in[:, cols], grad_hid[:, pl.ds(al((q // 2) * W, W), W)], 0, 0)
        up_store(q).start()

    def second_norm(q):
        rows = pl.ds(al(q * 64, 64), 64)
        upstream = part[rows, :] + land[rows, :]
        normed = (stream_one[rows, :] - mean_two[rows, 0:1]) * inv_two[rows, 0:1]
        low = two_low[rows, :].astype(f32)
        down_sum[0:1, :] = down_sum[0:1, :] + jnp.sum(low, axis=0, keepdims=True)
        grad = low + norm_back(upstream, normed, inv_two[rows, 0:1], gains[1:2, :])
        grad_one[rows, :] = grad
        one_low[rows, :] = grad.astype(bf16)
        add_sum(0, grad)
        add_sum(1, upstream * normed)
        add_sum(2, upstream)

    def into_heads(q):
        rows = pl.ds(al(q * 128, 128), 128)
        grad_att[rows, :] = mm(one_low[rows, :], out_w[...], 1, 1).astype(bf16)

    def attention(q):
        image, pair = q // 4, lax.rem(q, 4)
        rows, cols = pl.ds(al(image * slots, slots), slots), pl.ds(al(pair * 128, 128), 128)
        qs, ks, vs, gs = queries[rows, cols], keys[rows, cols], values[rows, cols], grad_att[rows, cols]
        keep = lax.broadcasted_iota(jnp.int32, (1, slots), 1) < lens[image]
        scale = 1.0 / math.sqrt(HD)
        dq, dk, dv = [], [], []
        for h in range(2):
            part_of = slice(h * HD, (h + 1) * HD)
            qh, kh, vh, gh = qs[:, part_of], ks[:, part_of], vs[:, part_of], gs[:, part_of]
            scores = jnp.where(keep, mm(qh, kh, 1, 1) * scale, -1e30)
            exps = jnp.exp(scores - jnp.max(scores, axis=-1, keepdims=True))
            probs = exps / jnp.sum(exps, axis=-1, keepdims=True)
            grad_probs = mm(gh, vh, 1, 1)
            dv.append(mm(probs.astype(bf16), gh, 0, 0))
            dot = jnp.sum(probs * grad_probs, axis=-1, keepdims=True)
            grad_scores = (probs * (grad_probs - dot)).astype(bf16)
            dq.append(mm(grad_scores, kh, 1, 0) * scale)
            dk.append(mm(grad_scores, qh, 0, 0) * scale)
        for at, pieces in enumerate((dq, dk, dv)):
            grad_proj[at, rows, cols] = jnp.concatenate(pieces, axis=1).astype(bf16)

    def into_norm(q):
        rows = pl.ds(al(q * 128, 128), 128)
        part[rows, :] = (
            mm(grad_proj[0, rows, :], qkv_w[0], 1, 1)
            + mm(grad_proj[1, rows, :], qkv_w[1], 1, 1)
            + mm(grad_proj[2, rows, :], qkv_w[2], 1, 1))

    def out_weight(q):
        cols = pl.ds(al(q * 128, 128), 128)
        tall[0:128, :] = mm(attended[:, cols], one_low[...], 0, 0)
        out_store(q).start()

    def proj_weight(q):
        which, block = q // 4, lax.rem(q, 4)
        cols = pl.ds(al(block * 256, 256), 256)
        wide[0:256, :] = mm(attn_in[:, cols], grad_proj[which], 0, 0)
        proj_store(q).start()

    def first_norm(q):
        rows = pl.ds(al(q * 64, 64), 64)
        upstream, normed = part[rows, :] + land_two[rows, :], normed_one[rows, :]
        grad = grad_one[rows, :] + norm_back(upstream, normed, inv_one[rows, 0:1], gains[0:1, :])
        zero_low[rows, :] = grad.astype(bf16)
        add_sum(3, upstream * normed)
        add_sum(4, upstream)
        add_sum(5, grad)

    def embed_weight(q):
        cols = pl.ds(al(q * 256, 256), 256)
        tall[...] = mm(pixel_low[:, cols], zero_low[...], 0, 0)
        embed_store(q).start()

    def pixels_back(q):
        rows = pl.ds(al(q * 128, 128), 128)
        grad = mm(zero_low[rows, :], embed_w[...], 1, 1)
        grad_pix[rows, :] = grad
        add_sum(6, grad)
        add_sum(7, grad * pixel_hat[rows, :])

    def pack(q):
        for col in range(blocks):
            small_grad[col : col + 1, :] = up_sum[0:1, col * W : (col + 1) * W]
        for col in range(2):
            small_grad[4 + col : 5 + col, :] = down_sum[0:1, col * W : (col + 1) * W]
        for row in range(8):
            small_grad[8 + 2 * row : 9 + 2 * row, :] = sums[row : row + 1, :W]
            small_grad[9 + 2 * row : 10 + 2 * row, :] = sums[row : row + 1, W:]
        for row, at in ((24, 0), (25, 2)):
            small_grad[row : row + 1, :] = jnp.sum(grad_proj[at].astype(f32), axis=0, keepdims=True)

    def keep_rows(q, height):
        at = lax.rem(q, slots // height) * height + lax.broadcasted_iota(jnp.int32, (height, 1), 0)
        return (at < lens[q // (slots // height)]).astype(f32)

    def layer_end(q):
        rows = pl.ds(al(q * 64, 64), 64)
        total_row = stream_one[rows, :] + (mlp_part[rows, :] + land[rows, :]) + down_bias[...]
        one_low[rows, :] = (total_row * keep_rows(q, 64)).astype(bf16)

    def pixel_end(q):
        rows = pl.ds(al(q * 128, 128), 128)
        keep = keep_rows(q, 128)
        first = jnp.concatenate([small_total[20:21, :], small_total[21:22, :]], axis=1)
        cross = jnp.concatenate([small_total[22:23, :], small_total[23:24, :]], axis=1)
        band = pixel_hat.shape[1] // 3
        for at in range(3):
            cols = slice(at * band, (at + 1) * band)
            a_sum = jnp.sum(first[:, cols], axis=1, keepdims=True)
            b_sum = jnp.sum(cross[:, cols], axis=1, keepdims=True)
            grad_pix[rows, cols] = stats[1:2, cols] * (
                grad_pix[rows, cols]
                - keep * (a_sum + b_sum * pixel_hat[rows, cols]) / stats[2:3, cols])

    def fetch_early(q):
        for at in range(5):
            fetches[at].wait()

    def fetch_late(q):
        for at in range(5, FETCH):
            fetches[at].wait()

    def act(method, *copies):
        def piece(q):
            for copy in copies:
                getattr(copy, method)()
        return piece

    def landed(store):
        return lambda q: store(q).wait()

    def shift(piece, by):
        return lambda q: piece(q + by)

    def weights(begin, number, piece, store, base=0):
        return (
            (begin + 1, number, shift(landed(store), base)), (begin, number, shift(piece, base)))

    plan = (
        (0, 1, fetch_early), (0, 4, feed),
        *weights(4, 2, down_weight, down_store), *weights(4, 2, up_weight, up_store),
        (7, 12, shift(feed, 4)), (19, 1, act("start", *first_sum)),
        *weights(19, 2, down_weight, down_store, 2), *weights(21, 2, up_weight, up_store, 2),
        *weights(23, 2, down_weight, down_store, 4), *weights(25, 2, up_weight, up_store, 4),
        *weights(27, 2, down_weight, down_store, 6), *weights(29, 2, up_weight, up_store, 6),
        (30, 1, fetch_late), (31, 1, act("wait", first_sum[0])), (31, 4, second_norm),
        (35, 2, into_heads), (37, 4, attention), (41, 2, into_norm),
        (42, 1, act("wait", first_sum[1])), (42, 4, shift(second_norm, 4)),
        (43, 1, act("start", second_sum[0])),
        (46, 2, shift(into_heads, 2)), (48, 4, shift(attention, 4)), (52, 2, shift(into_norm, 2)),
        (54, 1, act("start", second_sum[1])),
        (55, 1, act("wait", second_sum[0])), (55, 4, first_norm),
        *weights(56, 4, out_weight, out_store), *weights(58, 12, proj_weight, proj_store),
        (67, 1, act("wait", second_sum[1])), (67, 4, shift(first_norm, 4)),
        (68, 1, act("start", third_sum)),
        *weights(71, 3, embed_weight, embed_store), (75, 4, pixels_back), (79, 1, pack),
        (93, 1, act("wait", third_sum)), (93, 8, layer_end), (101, 1, act("start", layer_copy)),
        (117, 1, act("start", total_copy)), (118, 1, act("wait", total_copy)), (119, 4, pixel_end),
        (123, 1, act("start", pixel_copy)))
    first = 7
    per_block = 2 * (W // (2 * R)) * 2
    starts, total = [0, 0], 2 * per_block * blocks // 2
    for rows_of, cols_of in shapes[2:]:
        starts.append(total)
        total += (rows_of // (2 * R)) * (cols_of // W)
    NC = total

    def slot(j): return lax.rem(j, K)
    a_mine = al(x*Q, Q); a_other = al((1-x)*Q, Q)
    e_near = al(side*E, E); e_far = al((1-side)*E, E)
    b_near = al(H + side*Q, Q); b_far = al(H + (1-side)*Q, Q)
    aN = al(x*Q + side*E, E); aF = al(x*Q + (1-side)*E, E)
    def hbm(ref, a, j, half):
        if a == 0:
            block, q = j // per_block, lax.rem(j, per_block) - per_block // 2
            r, col = q * (2 * R) + half * R, block * W
        elif a == 1:
            block, q = j // per_block, lax.rem(j, per_block)
            r, col = block * W + (q // 2) * (2 * R) + half * R, lax.rem(q, 2) * W
        else:
            cols = shapes[a][1] // W
            q = j - starts[a]
            r, col = (q // cols) * (2 * R) + half * R, lax.rem(q, cols) * W
        return ref.at[pl.ds(al(r, R), R), pl.ds(al(col, W), W)]
    def rc(kind, src, dst, dev, s):
        k = SEND.index(kind)
        return pltpu.make_async_remote_copy(src_ref=src, dst_ref=dst, send_sem=ssem.at[k, s], recv_sem=rsem.at[k, s], device_id=dev, device_id_type=MESH)
    def desc(kind, j):
        s = slot(j)
        if kind == "x": return rc(kind, own.at[s, pl.ds(a_other, Q)], xl.at[s], dev_x, s)
        if kind == "ob": return rc(kind, own.at[s, pl.ds(H, H)], ob.at[s], dev_o, s)
        if kind == "oa": return rc(kind, ab.at[s], oa.at[s], dev_o, s)
        if kind == "ja": return rc(kind, ab.at[s, pl.ds(e_far, E)], ja.at[s], dev_j, s)
        if kind == "jb": return rc(kind, own.at[s, pl.ds(b_far, Q)], jb.at[s], dev_j, s)
        if kind == "xb": return rc(kind, nbuf.at[s], xbl.at[s], dev_x, s)
        if kind in ("ga", "na"):
            return rc(kind, fin.at[s, pl.ds(aN, E)], fin.at[s, pl.ds(aN, E)], dev_j if kind == "ga" else dev_o, s)
        if kind == "fa": return rc(kind, fin.at[s, pl.ds(aF, E)], fin.at[s, pl.ds(aF, E)], dev_o, s)
        if kind in ("gb", "nb"):
            return rc(kind, fin.at[s, pl.ds(b_near, Q)], fin.at[s, pl.ds(b_near, Q)], dev_j if kind == "gb" else dev_o, s)
        if kind == "fb": return rc(kind, fin.at[s, pl.ds(b_far, Q)], fin.at[s, pl.ds(b_far, Q)], dev_o, s)
        if kind == "xg": return rc(kind, fin.at[s, pl.ds(a_mine, Q)], fin.at[s, pl.ds(a_mine, Q)], dev_x, s)
        if kind == "c": return rc(kind, ins[0].at[pl.ds(0, R), pl.ds(0, W)], cl.at[s], dev_c, s)
        if kind == "cg": return rc(kind, fin.at[s], outs[0].at[pl.ds(0, R), pl.ds(0, W)], dev_c, s)
        raise ValueError(kind)
    def each(j, f):
        for a in range(n):
            if a < 2:
                late = lax.rem(j, per_block) >= per_block // 2
                cond = (j < starts[2]) & (late if a == 0 else jnp.logical_not(late))
            else:
                cond = (j >= starts[a]) & (j < (starts[a + 1] if a + 1 < n else NC))
            pl.when(cond)(functools.partial(f, a))
    d = delays
    def step(tt, carry):
        js = [tt - first - dd for dd in d]
        def on(k): return (js[k] >= 0) & (js[k] < NC)
        @pl.when(on(7))
        def _():
            j = js[7]; s = slot(j)
            pltpu.make_async_copy(fin.at[s], outs[0].at[pl.ds(0, R), pl.ds(0, W)], lsem.at[1, s]).wait()
            desc("cg", j).wait_send(); desc("cg", j).wait_recv()
            desc("c", j).wait_send(); desc("x", j).wait_send(); desc("xg", j).wait_send()
            @pl.when(outer)
            def _():
                desc("oa", j).wait_send(); desc("ob", j).wait_send()
            @pl.when(inner)
            def _():
                for k in ("ja","jb","xb","ga","gb","na","fa","nb","fb"): desc(k, j).wait_send()
        @pl.when(on(6))
        def _():
            j = js[6]
            desc("xg", j).wait_recv()
            @pl.when(outer)
            def _():
                desc("nb", j).wait_recv(); desc("fb", j).wait_recv()
        @pl.when(on(5))
        def _():
            j = js[5]
            @pl.when(inner)
            def _():
                desc("ga", j).wait_recv(); desc("gb", j).wait_recv()
        j5o = tt - first - d[5] - d[8]
        on5o = (j5o >= 0) & (j5o < NC)
        @pl.when(on5o & outer)
        def _():
            desc("na", j5o).wait_recv(); desc("fa", j5o).wait_recv()
        @pl.when(on(4))
        def _():
            j = js[4]; s = slot(j)
            @pl.when(inner)
            def _():
                desc("ja", j).wait_recv(); desc("xb", j).wait_recv()
                fin[s, pl.ds(aN, E)] = ab[s, pl.ds(e_near, E)] + ja[s]
                fin[s, pl.ds(b_near, Q)] = nbuf[s] + xbl[s]
        @pl.when(on(3))
        def _():
            j = js[3]; s = slot(j)
            @pl.when(inner)
            def _():
                desc("oa", j).wait_recv(); desc("jb", j).wait_recv()
                ab[s] = ab[s] + oa[s]
                nbuf[s] = own[s, pl.ds(b_near, Q)] + jb[s]
        @pl.when(on(2))
        def _():
            j = js[2]; s = slot(j)
            desc("x", j).wait_recv()
            ab[s] = own[s, pl.ds(a_mine, Q)] + xl[s]
            @pl.when(inner)
            def _():
                desc("ob", j).wait_recv()
                own[s, pl.ds(H, H)] = own[s, pl.ds(H, H)] + ob[s]
        @pl.when(on(1))
        def _():
            j = js[1]; s = slot(j)
            pltpu.make_async_copy(ins[0].at[pl.ds(0, R), pl.ds(0, W)], own.at[s], lsem.at[0, s]).wait()
            desc("c", j).wait_recv()
            own[s] = own[s] + cl[s]
        @pl.when(on(6))
        def _():
            j = js[6]; s = slot(j)
            def f(a):
                pltpu.make_async_copy(fin.at[s], hbm(outs[a], a, j, c), lsem.at[1, s]).start()
                rc("cg", fin.at[s], hbm(outs[a], a, j, c), dev_c, s).start()
            each(j, f)
        @pl.when(on(5))
        def _():
            j = js[5]
            @pl.when(inner)
            def _():
                desc("fa", j).start(); desc("xg", j).start(); desc("fb", j).start()
        @pl.when(on5o & outer)
        def _():
            desc("xg", j5o).start()
        @pl.when(on(4))
        def _():
            j = js[4]
            @pl.when(inner)
            def _():
                for k in ("ga","na","gb","nb"): desc(k, j).start()
        @pl.when(on(3))
        def _():
            j = js[3]
            @pl.when(inner)
            def _():
                desc("ja", j).start(); desc("xb", j).start()
        @pl.when(on(2))
        def _():
            j = js[2]
            @pl.when(outer)
            def _(): desc("oa", j).start()
            @pl.when(inner)
            def _(): desc("jb", j).start()
        @pl.when(on(1))
        def _():
            j = js[1]
            desc("x", j).start()
            @pl.when(outer)
            def _(): desc("ob", j).start()
        @pl.when(on(0))
        def _():
            j = js[0]; s = slot(j)
            def f(a):
                pltpu.make_async_copy(hbm(ins[a], a, j, c), own.at[s], lsem.at[0, s]).start()
                rc("c", hbm(ins[a], a, j, 1 - c), cl.at[s], dev_c, s).start()
            each(j, f)
        for begin, number, piece in plan:
            if number == 1:
                pl.when(tt == begin)(functools.partial(piece, 0))
            else:
                pl.when((tt >= begin) & (tt < begin + number))(functools.partial(piece, tt - begin))
        return carry
    lax.fori_loop(0, first + NC + d[7], step, 0)
    layer_copy.wait()
    pixel_copy.wait()


def back_pass(lengths, fetched, R=64, K=14, delays=(0, 1, 3, 5, 7, 9, 12, 13, 1)):
    f32, bf16 = jnp.float32, jnp.bfloat16
    tokens, width = fetched[0].shape
    hidden = fetched[1].shape[1]
    local = fetched[8].shape[1]
    patch = fetched[17].shape[1]
    shapes = (
        (width, hidden), (hidden, width), (local, width), (3 * width, local), (2 * R, W), (patch, width))
    n = len(shapes)
    H, Q, E = R // 2, R // 4, R // 8
    V = lambda r: pltpu.VMEM((K, r, W), f32)
    anywhere = pl.BlockSpec(memory_space=pl.ANY)
    held = [pltpu.VMEM(a.shape, a.dtype) for a in fetched]
    out = [jax.ShapeDtypeStruct(s, f32) for s in shapes]
    out += [jax.ShapeDtypeStruct(s, f32) for s in shapes[:4] + shapes[5:]]
    out += [jax.ShapeDtypeStruct((tokens, width), bf16), jax.ShapeDtypeStruct((tokens, patch), f32)]
    stream = pltpu.VMEM((tokens, width), f32)
    narrow = pltpu.VMEM((tokens, width), bf16)
    results = pl.pallas_call(
        functools.partial(back_kernel, shapes, R, K, delays),
        out_shape=out,
        in_specs=[pl.BlockSpec(memory_space=pltpu.SMEM)] + [anywhere] * FETCH,
        out_specs=[anywhere] * len(out),
        scratch_shapes=[
            *held,
            stream, stream, stream, stream, stream, narrow, narrow,
            pltpu.VMEM((tokens, local), bf16), pltpu.VMEM((3, tokens, local), bf16),
            pltpu.VMEM((tokens, patch), f32), pltpu.VMEM((tokens, hidden), bf16),
            pltpu.VMEM((tokens, hidden), bf16), pltpu.VMEM((8, width), f32),
            pltpu.VMEM((1, hidden), f32), pltpu.VMEM((1, width), f32), pltpu.VMEM(shapes[4], f32),
            pltpu.VMEM((32, W), f32), pltpu.VMEM((256, width), f32), pltpu.VMEM((512, W), f32),
            V(R), V(R), V(Q), V(Q), V(Q), V(H), V(E), V(Q), V(Q), V(Q), V(R),
            pltpu.SemaphoreType.DMA((len(SEND), K)), pltpu.SemaphoreType.DMA((len(SEND), K)),
            pltpu.SemaphoreType.DMA((2, K)), pltpu.SemaphoreType.DMA((FETCH,)),
            pltpu.SemaphoreType.DMA((8,)), pltpu.SemaphoreType.DMA((5,)), pltpu.SemaphoreType.DMA((5,)),
        ],
        compiler_params=pltpu.CompilerParams(
            collective_id=1, has_side_effects=True, vmem_limit_bytes=67_000_000),
        name="back_pass")(lengths, *fetched)
    return (*results[:n], *results[-2:])


def stats_kernel(ranks, band_width, lens, pix, out, mine, table, ssem, rsem):
    me = lax.axis_index("dp")
    t = lax.axis_index("tensor")
    bar = pltpu.get_barrier_semaphore()
    for k in range(1, ranks):
        pl.semaphore_signal(bar, inc=1, device_id=(lax.rem(me + k, ranks), t), device_id_type=MESH)
    images, slots, width = pix.shape
    one = jnp.zeros((1, width), jnp.float32)
    two = jnp.zeros((1, width), jnp.float32)
    number = jnp.zeros((1, width), jnp.float32)
    for k in range(images):
        keep = (lax.broadcasted_iota(jnp.int32, (slots, 1), 0) < lens[k]).astype(jnp.float32)
        x = pix[k].astype(jnp.float32)
        kept = x * keep
        one = one + jnp.sum(kept, axis=0, keepdims=True)
        two = two + jnp.sum(kept * x, axis=0, keepdims=True)
        number = number + jnp.sum(keep, axis=0, keepdims=True)
    folded = []
    for line in (one, two):
        for b in range(3):
            at = b * band_width
            folded.append(
                sum(line[:, at + lane : at + lane + 128] for lane in range(0, band_width, 128)))
    folded += [number[:, :128], jnp.zeros((1, 128), jnp.float32)]
    mine[...] = jnp.concatenate(folded, axis=0)
    pl.semaphore_wait(bar, ranks - 1)

    def copy(k):
        peer = lax.rem(me + k, ranks)
        return pltpu.make_async_remote_copy(
            src_ref=mine, dst_ref=table.at[me], send_sem=ssem.at[k - 1], recv_sem=rsem.at[me],
            device_id=(peer, t), device_id_type=MESH)

    def arrival(k):
        peer = lax.rem(me + k, ranks)
        return pltpu.make_async_remote_copy(
            src_ref=mine, dst_ref=table.at[peer], send_sem=ssem.at[k - 1], recv_sem=rsem.at[peer],
            device_id=(peer, t), device_id_type=MESH)

    for k in range(1, ranks):
        copy(k).start()
    table[me] = mine[...]
    for k in range(1, ranks):
        arrival(k).wait_recv()
    total = table[0]
    for k in range(1, ranks):
        total = total + table[k]
    for k in range(1, ranks):
        copy(k).wait_send()
    for b in range(width // band_width):
        cols = slice(b * band_width, (b + 1) * band_width)
        count = jnp.concatenate([total[6:7, :]] * (band_width // 128), axis=1) * float(band_width)
        mean = jnp.sum(total[b : b + 1, :], axis=1, keepdims=True) / count
        square = jnp.sum(total[3 + b : 4 + b, :], axis=1, keepdims=True) / count
        rstd = lax.rsqrt(square - mean * mean + 1e-05)
        out[:, cols] = jnp.concatenate(
            [mean, rstd, count, jnp.zeros((5, band_width), jnp.float32)], axis=0)


def band_stats(pixels, lengths, ranks):
    width = pixels.shape[2]
    return pl.pallas_call(
        functools.partial(stats_kernel, ranks, width // 3),
        out_shape=jax.ShapeDtypeStruct((8, width), jnp.float32),
        in_specs=[pl.BlockSpec(memory_space=pltpu.SMEM), pl.BlockSpec(memory_space=pltpu.VMEM)],
        out_specs=pl.BlockSpec(memory_space=pltpu.VMEM),
        scratch_shapes=[
            pltpu.VMEM((8, 128), jnp.float32),
            pltpu.VMEM((ranks, 8, 128), jnp.float32),
            pltpu.SemaphoreType.DMA((ranks,)),
            pltpu.SemaphoreType.DMA((ranks,)),
        ],
        compiler_params=pltpu.CompilerParams(collective_id=2, has_side_effects=True),
        name="band_stats")(lengths, pixels)


def positions(patch_ids, gsd_values, model_width, grid_side):
    quarter = model_width // 4
    gsd_scale = gsd_values.astype(jnp.float32) / 100.0
    row_pos = (patch_ids // grid_side).astype(jnp.float32) * gsd_scale[:, None]
    col_pos = (patch_ids % grid_side).astype(jnp.float32) * gsd_scale[:, None]
    frequency = jnp.exp(jnp.arange(quarter, dtype=jnp.float32) * (-math.log(10000.0) / quarter))
    row_angle = row_pos[:, :, None] * frequency
    col_angle = col_pos[:, :, None] * frequency
    return jnp.concatenate(
        [jnp.sin(row_angle), jnp.cos(row_angle), jnp.sin(col_angle), jnp.cos(col_angle)], axis=-1
    )


def contract_rows(left_side, right_side):
    return lax.dot_general(
        left_side, right_side, (((0,), (0,)), ((), ())), preferred_element_type=jnp.float32
    )


def contract_cols(left_side, right_side):
    return lax.dot_general(
        left_side, right_side, (((1,), (1,)), ((), ())), preferred_element_type=jnp.float32
    )


def normalize(hidden, gain_row, shift_row):
    centred = hidden - jnp.mean(hidden, axis=-1, keepdims=True)
    inverse = lax.rsqrt(jnp.mean(centred * centred, axis=-1, keepdims=True) + 1e-06)
    normed = centred * inverse
    return (normed * gain_row + shift_row, normed, inverse)


def normalize_back(upstream, normed, inverse, gain_row):
    scaled = upstream * gain_row
    return inverse * (
        scaled
        - jnp.mean(scaled, axis=-1, keepdims=True)
        - normed * jnp.mean(scaled * normed, axis=-1, keepdims=True)
    )


def gelu_slope(inputs):
    return 0.5 * (1.0 + lax.erf(inputs * (1.0 / math.sqrt(2.0)))) + inputs * jnp.exp(
        -0.5 * inputs * inputs
    ) * (1.0 / math.sqrt(2.0 * math.pi))


def tensor_sum(part):
    if lax.axis_size("tensor") != 2:
        return lax.psum(part, "tensor")
    return part + lax.ppermute(part, "tensor", [(0, 1), (1, 0)])


def per_device(
    fast,
    pixels,
    lengths,
    patch_ids,
    gsd_values,
    embed_w,
    embed_bias,
    norm_gain,
    norm_bias,
    qkv_w,
    qv_bias,
    out_w,
    out_bias,
    up_w,
    up_bias,
    down_w,
    down_bias,
    cotangent,
):
    images, slot_count, patch_width = pixels.shape
    band_width = patch_width // 3
    model_width = embed_w.shape[1]
    local_width = qkv_w.shape[2]
    head_dim = HD
    heads_here = local_width // head_dim
    tokens = images * slot_count
    score_scale = 1.0 / math.sqrt(head_dim)
    key_keep = jnp.arange(slot_count)[None, :] < lengths[:, None]
    valid_rows = key_keep.astype(jnp.float32)
    pixel_grid = pixels.astype(jnp.float32).reshape(images, slot_count, 3, band_width)
    pixel_mask = valid_rows[:, :, None, None]
    if fast:
        stats = band_stats(pixels, lengths, 16)
        band_mean = stats[0].reshape(3, band_width)[:, 0]
        band_rstd = stats[1].reshape(3, band_width)[:, 0]
        band_count = stats[2, 0]
    else:
        total_one, total_two, band_count = lax.psum(
            (
                jnp.sum(pixel_grid * pixel_mask, axis=(0, 1, 3)),
                jnp.sum(pixel_grid * pixel_grid * pixel_mask, axis=(0, 1, 3)),
                jnp.sum(valid_rows) * band_width,
            ),
            "dp",
        )
        band_mean = total_one / band_count
        band_rstd = lax.rsqrt(total_two / band_count - band_mean * band_mean + 1e-05)
    pixel_hat = (pixel_grid - band_mean[:, None]) * band_rstd[:, None]
    pixel_low = pixel_hat.reshape(tokens, patch_width).astype(jnp.bfloat16)
    pos_table = positions(patch_ids, gsd_values, model_width, GRID).reshape(tokens, model_width)
    stream_zero = (
        jnp.dot(pixel_low, embed_w, preferred_element_type=jnp.float32) + embed_bias + pos_table
    )
    layer_one, normed_one, inverse_one = normalize(stream_zero, norm_gain[0], norm_bias[0])
    attn_input = layer_one.astype(jnp.bfloat16)
    queries = (
        jnp.dot(attn_input, qkv_w[0], preferred_element_type=jnp.float32) + qv_bias[0]
    ).astype(jnp.bfloat16)
    key_rows = jnp.dot(attn_input, qkv_w[1], preferred_element_type=jnp.float32).astype(
        jnp.bfloat16
    )
    values = (
        jnp.dot(attn_input, qkv_w[2], preferred_element_type=jnp.float32) + qv_bias[1]
    ).astype(jnp.bfloat16)
    query_heads = queries.reshape(images, slot_count, heads_here, head_dim)
    key_heads = key_rows.reshape(images, slot_count, heads_here, head_dim)
    value_heads = values.reshape(images, slot_count, heads_here, head_dim)

    def score_block():
        scores = (
            jnp.einsum(
                "ichd,ijhd->ihcj", query_heads, key_heads, preferred_element_type=jnp.float32
            )
            * score_scale
        )
        return jnp.where(key_keep[:, None, None, :], scores, -1e30)

    scores = score_block()
    top_score = jnp.max(scores, axis=-1, keepdims=True)
    exp_scores = jnp.exp(scores - top_score)
    exp_total = jnp.sum(exp_scores, axis=-1, keepdims=True)
    log_total = top_score + jnp.log(exp_total)
    prob_low = (exp_scores / exp_total).astype(jnp.bfloat16)
    attended = (
        jnp.einsum("ihcj,ijhd->ichd", prob_low, value_heads, preferred_element_type=jnp.float32)
        .astype(jnp.bfloat16)
        .reshape(tokens, local_width)
    )
    attn_out = tensor_sum(jnp.dot(attended, out_w, preferred_element_type=jnp.float32))
    stream_one = stream_zero + attn_out + out_bias
    layer_two, normed_two, inverse_two = normalize(stream_one, norm_gain[1], norm_bias[1])
    mlp_input = layer_two.astype(jnp.bfloat16)
    row_valid = valid_rows.reshape(tokens, 1)
    if fast:
        spread = lambda column: jnp.broadcast_to(column, (tokens, 128))
        two_low = cotangent.reshape(tokens, model_width) * row_valid.astype(jnp.bfloat16)
        mean_two = jnp.mean(stream_one, axis=-1, keepdims=True)
        fetched = (
            mlp_input, up_w, down_w, up_bias.reshape(1, -1), two_low, stream_one, spread(mean_two),
            spread(inverse_two), attended, out_w, queries, key_rows, values, attn_input, qkv_w, normed_one,
            spread(inverse_one), pixel_low, pixel_hat.reshape(tokens, patch_width), embed_w, norm_gain,
            down_bias.reshape(1, -1), stats)
        sum_up, sum_down, sum_out_proj, sum_qkv, small, embed_sum, output, pixel_grad = back_pass(
            lengths, fetched)
        rows = small[8:24].reshape(8, 2 * W)
        return (
            output.reshape(images, slot_count, model_width),
            pixel_grad.reshape(images, slot_count, patch_width),
            embed_sum,
            rows[5],
            jnp.stack([rows[3], rows[1]]),
            jnp.stack([rows[4], rows[2]]),
            sum_qkv.reshape(3, model_width, local_width),
            small[24:26],
            sum_out_proj,
            rows[0],
            sum_up,
            small[0:4].reshape(-1),
            sum_down,
            small[4:6].reshape(-1),
        )
    hidden_pre = jnp.dot(mlp_input, up_w, preferred_element_type=jnp.float32) + up_bias
    hidden_low = jax.nn.gelu(hidden_pre, approximate=False).astype(jnp.bfloat16)
    mlp_part = jnp.dot(hidden_low, down_w, preferred_element_type=jnp.float32)
    row_valid = valid_rows.reshape(tokens, 1)
    grad_two = cotangent.astype(jnp.float32).reshape(tokens, model_width) * row_valid
    grad_down_bias = jnp.sum(grad_two, axis=0)
    grad_two_low = grad_two.astype(jnp.bfloat16)
    grad_down = contract_rows(hidden_low, grad_two_low)
    grad_hidden = (contract_cols(grad_two_low, down_w) * gelu_slope(hidden_pre)).astype(
        jnp.bfloat16
    )
    grad_up = contract_rows(mlp_input, grad_hidden)
    grad_up_bias = jnp.sum(grad_hidden.astype(jnp.float32), axis=0)
    grad_mlp_in = tensor_sum(contract_cols(grad_hidden, up_w))
    grad_one = grad_two + normalize_back(grad_mlp_in, normed_two, inverse_two, norm_gain[1])
    grad_out_bias = jnp.sum(grad_one, axis=0)
    grad_one_low = grad_one.astype(jnp.bfloat16)
    grad_out_proj = contract_rows(attended, grad_one_low)
    grad_attended = (
        contract_cols(grad_one_low, out_w)
        .astype(jnp.bfloat16)
        .reshape(images, slot_count, heads_here, head_dim)
    )
    attn_probs = jnp.exp(score_block() - log_total)
    grad_probs = jnp.einsum(
        "ichd,ijhd->ihcj", grad_attended, value_heads, preferred_element_type=jnp.float32
    )
    grad_values = jnp.einsum(
        "ihcj,ichd->ijhd",
        attn_probs.astype(jnp.bfloat16),
        grad_attended,
        preferred_element_type=jnp.float32,
    ).astype(jnp.bfloat16)
    prob_dot = jnp.sum(attn_probs * grad_probs, axis=-1, keepdims=True)
    grad_scores = (attn_probs * (grad_probs - prob_dot)).astype(jnp.bfloat16)
    grad_queries = (
        jnp.einsum("ihcj,ijhd->ichd", grad_scores, key_heads, preferred_element_type=jnp.float32)
        * score_scale
    ).astype(jnp.bfloat16)
    grad_keys = (
        jnp.einsum("ihcj,ichd->ijhd", grad_scores, query_heads, preferred_element_type=jnp.float32)
        * score_scale
    ).astype(jnp.bfloat16)
    grad_proj = (
        grad_queries.reshape(tokens, local_width),
        grad_keys.reshape(tokens, local_width),
        grad_values.reshape(tokens, local_width),
    )
    grad_qkv = jnp.stack([contract_rows(attn_input, grad_piece) for grad_piece in grad_proj])
    grad_qv_bias = jnp.stack(
        [
            jnp.sum(grad_proj[0].astype(jnp.float32), axis=0),
            jnp.sum(grad_proj[2].astype(jnp.float32), axis=0),
        ]
    )
    attn_partial = (
        contract_cols(grad_proj[0], qkv_w[0])
        + contract_cols(grad_proj[1], qkv_w[1])
        + contract_cols(grad_proj[2], qkv_w[2])
    )
    grad_attn_in = tensor_sum(attn_partial)
    mlp_part, _ = lax.optimization_barrier((mlp_part, grad_attn_in))
    stream_two = stream_one + tensor_sum(mlp_part) + down_bias
    output = (stream_two * row_valid).astype(jnp.bfloat16).reshape(images, slot_count, model_width)
    grad_zero = grad_one + normalize_back(grad_attn_in, normed_one, inverse_one, norm_gain[0])
    grad_norm_gain = jnp.stack(
        [jnp.sum(grad_attn_in * normed_one, axis=0), jnp.sum(grad_mlp_in * normed_two, axis=0)]
    )
    grad_norm_bias = jnp.stack([jnp.sum(grad_attn_in, axis=0), jnp.sum(grad_mlp_in, axis=0)])
    grad_embed_bias = jnp.sum(grad_zero, axis=0)
    grad_zero_low = grad_zero.astype(jnp.bfloat16)
    embed_part = contract_rows(pixel_low, grad_zero_low)
    grad_pixel_hat = contract_cols(grad_zero_low, embed_w).reshape(
        images, slot_count, 3, band_width
    )
    band_grad = jnp.sum(grad_pixel_hat, axis=(0, 1, 3))
    band_cross = jnp.sum(grad_pixel_hat * pixel_hat, axis=(0, 1, 3))
    small = (
        grad_qv_bias,
        grad_out_bias,
        grad_up_bias,
        grad_down_bias,
        grad_norm_gain,
        grad_norm_bias,
        grad_embed_bias,
        band_grad,
        band_cross,
    )
    large = (grad_qkv.reshape(-1, local_width), grad_out_proj, grad_up, grad_down, embed_part)
    large, small = lax.psum((large, small), "dp")
    sum_qkv, sum_out_proj, sum_up, sum_down, embed_sum = large
    sum_qkv = sum_qkv.reshape(grad_qkv.shape)
    (
        sum_qv_bias,
        sum_out_bias,
        sum_up_bias,
        sum_down_bias,
        sum_gain,
        sum_shift,
        sum_embed_bias,
        band_grad_sum,
        band_cross_sum,
    ) = small
    pixel_grad = band_rstd[:, None] * (
        grad_pixel_hat
        - pixel_mask * (band_grad_sum[:, None] + band_cross_sum[:, None] * pixel_hat) / band_count
    )
    pixel_grad = pixel_grad.reshape(images, slot_count, patch_width)
    return (
        output,
        pixel_grad,
        embed_sum,
        sum_embed_bias,
        sum_gain,
        sum_shift,
        sum_qkv,
        sum_qv_bias,
        sum_out_proj,
        sum_out_bias,
        sum_up,
        sum_up_bias,
        sum_down,
        sum_down_bias,
    )


def solution(mesh):
    fast = dict(mesh.shape) == {"dp": 16, "tensor": 2}
    in_specs = (
        P("dp", None, None),
        P("dp"),
        P("dp", None),
        P("dp"),
        P(),
        P(),
        P(),
        P(),
        P(None, None, "tensor"),
        P(None, "tensor"),
        P("tensor", None),
        P(),
        P(None, "tensor"),
        P("tensor"),
        P("tensor", None),
        P(),
        P("dp", None, None),
    )
    out_specs = (
        P("dp", None, None),
        P("dp", None, None),
        P(),
        P(),
        P(),
        P(),
        P(None, None, "tensor"),
        P(None, "tensor"),
        P("tensor", None),
        P(),
        P(None, "tensor"),
        P("tensor"),
        P("tensor", None),
        P(),
    )
    return jax.shard_map(
        functools.partial(per_device, fast), mesh=mesh, in_specs=in_specs, out_specs=out_specs, check_vma=False
    )
```

```python
import functools
import math

import jax
import jax.numpy as jnp
from jax import lax
from jax.experimental import pallas as pl
from jax.experimental.pallas import tpu as pltpu
from jax.sharding import PartitionSpec as P

HD = 64
GRID = 28
MESH = pl.DeviceIdType.MESH
W = 512


SEND = (
    "c","x","oa","ob","ja","jb","xb","ga","gb","na","fa","nb","fb","xg","cg")

FETCH = 25


def back_kernel(shapes, R, K, delays, *refs):
    n = len(shapes)
    lens = refs[0]
    fetched = refs[1 : 1 + FETCH]
    outs = refs[1 + FETCH : 1 + FETCH + n]
    ins = refs[1 + FETCH + n : 1 + FETCH + 2 * n - 1]
    layer_out, pixel_out = refs[FETCH + 2 * n : FETCH + 2 * n + 2]
    scratch = refs[FETCH + 2 * n + 2 :]
    held, scratch = scratch[: FETCH - 3], scratch[FETCH - 3 :]
    (attended, out_w, stream_one, gains, shifts, out_bias, up_w, down_w, up_bias, two_low, queries,
     keys, values, attn_in, qkv_w, normed_one, inv_one, pixel_low, pixel_hat, embed_w, down_bias,
     stats) = held
    (part, mlp_part, land, land_two, grad_one, one_low, zero_low, grad_att, grad_proj, grad_pix, hidden,
     grad_hid, sums, up_sum, down_sum, small_grad, small_total, tall, wide, land_att, mlp_in, mean_two,
     inv_two) = scratch[:23]
    own, cl, xl, ab, oa, ob, ja, jb, nbuf, xbl, fin, ssem, rsem, lsem, fsem, wsem, ysend, yrecv = scratch[23:]
    ins = (*ins[:4], small_grad, ins[4])
    slots = normed_one.shape[0] // 2
    blocks = hidden.shape[1] // W
    H, Q, E = R//2, R//4, R//8
    i = lax.axis_index("dp"); t = lax.axis_index("tensor")
    c = lax.rem(i, 2); x = lax.rem(i//2, 2); z = i//4
    side = z//2
    pos = lax.rem(z, 2)
    inner = lax.rem(side + pos, 2) == 1
    outer = lax.rem(side + pos, 2) == 0
    dev_c = (z*4 + x*2 + 1 - c, t)
    dev_x = (z*4 + (1-x)*2 + c, t)
    dev_o = ((side*2 + 1 - pos)*4 + x*2 + c, t)
    dev_j = ((3 - z)*4 + x*2 + c, t)
    dev_y = (i, 1 - t)
    att_wide, near_w, mate_w = fetched[FETCH - 3 :]
    half_rows = near_w.shape[0]
    fetches = [
        pltpu.make_async_copy(
            near_w, land_two.at[pl.ds(pl.multiple_of(c * half_rows, half_rows), half_rows)], fsem.at[FETCH - 2]),
        pltpu.make_async_copy(
            mate_w, land_two.at[pl.ds(pl.multiple_of((1 - c) * half_rows, half_rows), half_rows)],
            fsem.at[FETCH - 1])]
    fetches += [pltpu.make_async_copy(fetched[q], held[q], fsem.at[q]) for q in range(FETCH - 3)]
    for q in fetches:
        q.start()
    bar = pltpu.get_barrier_semaphore()
    for d in (dev_c, dev_x, dev_o, dev_y):
        pl.semaphore_signal(bar, inc=1, device_id=d, device_id_type=MESH)
    @pl.when(inner)
    def _():
        pl.semaphore_signal(bar, inc=1, device_id=dev_j, device_id_type=MESH)
        pl.semaphore_wait(bar, 5)
    @pl.when(outer)
    def _():
        pl.semaphore_wait(bar, 4)
    def al(v, m): return pl.multiple_of(v, m)

    def across(q, src, dst):
        return pltpu.make_async_remote_copy(
            src_ref=src, dst_ref=dst, send_sem=ysend.at[q], recv_sem=yrecv.at[q],
            device_id=dev_y, device_id_type=MESH)

    def image_rows(q):
        return pl.ds(q * slots, slots)

    first_sum = [across(q, part.at[image_rows(q)], land.at[image_rows(q)]) for q in range(2)]
    second_sum = [across(2 + q, part.at[image_rows(q)], land_two.at[image_rows(q)]) for q in range(2)]
    third_sum = across(4, mlp_part, land)
    heads_sum = [
        across(5 + q, att_wide.at[pl.ds(q * 128, 128)], land_att.at[pl.ds(q * 128, 128)]) for q in range(4)]
    for q in heads_sum:
        q.start()
    pixel_copy = pltpu.make_async_copy(grad_pix, pixel_out, wsem.at[5])
    layer_copy = pltpu.make_async_copy(one_low, layer_out, wsem.at[6])
    total_copy = pltpu.make_async_copy(outs[4].at[pl.ds(0, 32)], small_total, wsem.at[7])
    sums[...] = jnp.zeros_like(sums)
    small_grad[...] = jnp.zeros_like(small_grad)
    up_sum[...] = jnp.zeros_like(up_sum)
    down_sum[...] = jnp.zeros_like(down_sum)
    f32, bf16 = jnp.float32, jnp.bfloat16

    def mm(a, b, ca, cb):
        return lax.dot_general(a, b, (((ca,), (cb,)), ((), ())), preferred_element_type=f32)

    def add_sum(row, value):
        width = value.shape[1]
        sums[row : row + 1, :width] = sums[row : row + 1, :width] + jnp.sum(value, axis=0, keepdims=True)

    def norm_back(upstream, normed, inverse, gain_row):
        scaled = upstream * gain_row
        return inverse * (
            scaled
            - jnp.mean(scaled, axis=-1, keepdims=True)
            - normed * jnp.mean(scaled * normed, axis=-1, keepdims=True))

    def project(q):
        pl.when(q == 0)(lambda: wait_tile(0))
        for tile in range(1, 4):
            pl.when(q == tile)(functools.partial(wait_tile, tile))
        rows = pl.ds(al(q * 128, 128), 128)
        total_row = mm(attended[rows, :], out_w[...], 1, 0) + mm(
            land_att[rows, :].astype(bf16), zero_low[...], 1, 0)
        row = stream_one[rows, :] + total_row + out_bias[...]
        mean = jnp.mean(row, axis=-1, keepdims=True)
        centred = row - mean
        inverse = lax.rsqrt(jnp.mean(centred * centred, axis=-1, keepdims=True) + 1e-06)
        stream_one[rows, :] = row
        mean_two[rows, :] = jnp.broadcast_to(mean, (128, 128))
        inv_two[rows, :] = jnp.broadcast_to(inverse, (128, 128))
        mlp_in[rows, :] = (centred * inverse * gains[1:2, :] + shifts[1:2, :]).astype(bf16)

    def wait_tile(tile):
        heads_sum[tile].wait()

    def feed(q):
        block, rows = q // 4, pl.ds(al(lax.rem(q, 4) * 128, 128), 128)
        cols = pl.ds(al(block * W, W), W)
        low = two_low[rows, :]
        up_block, down_block = up_w[:, cols], down_w[cols, :]
        u = mm(mlp_in[rows, :], up_block, 1, 0) + up_bias[0:1, cols]
        below = 0.5 * (1.0 + lax.erf(u * (1.0 / math.sqrt(2.0))))
        hid = (u * below).astype(bf16)
        slope = below + u * jnp.exp(-0.5 * u * u) * (1.0 / math.sqrt(2.0 * math.pi))
        grad = (mm(low, down_block, 1, 1) * slope).astype(bf16)
        hidden[rows, cols] = hid
        grad_hid[rows, cols] = grad
        up_sum[0:1, cols] = up_sum[0:1, cols] + jnp.sum(grad.astype(f32), axis=0, keepdims=True)
        to_in, to_out = mm(grad, up_block, 1, 1), mm(hid, down_block, 1, 0)

        @pl.when(block == 0)
        def _():
            part[rows, :] = to_in
            mlp_part[rows, :] = to_out

        @pl.when(block > 0)
        def _():
            part[rows, :] = part[rows, :] + to_in
            mlp_part[rows, :] = mlp_part[rows, :] + to_out

    def down_store(q):
        return pltpu.make_async_copy(tall, ins[1].at[pl.ds(al(q * 256, 256), 256)], wsem.at[0])

    def up_store(q):
        rows = pl.ds(al(lax.rem(q, 2) * 512, 512), 512)
        return pltpu.make_async_copy(wide, ins[0].at[rows, pl.ds(al((q // 2) * W, W), W)], wsem.at[1])

    def out_store(q):
        return pltpu.make_async_copy(
            tall.at[pl.ds(0, 128)], ins[2].at[pl.ds(al(q * 128, 128), 128)], wsem.at[2])

    def proj_store(q):
        return pltpu.make_async_copy(
            wide.at[pl.ds(0, 256)], ins[3].at[pl.ds(al(q * 256, 256), 256)], wsem.at[3])

    def embed_store(q):
        return pltpu.make_async_copy(tall, ins[5].at[pl.ds(al(q * 256, 256), 256)], wsem.at[4])

    def down_weight(q):
        tall[...] = mm(hidden[:, pl.ds(al(q * 256, 256), 256)], two_low[...], 0, 0)
        down_store(q).start()

    def up_weight(q):
        cols = pl.ds(al(lax.rem(q, 2) * 512, 512), 512)
        wide[...] = mm(mlp_in[:, cols], grad_hid[:, pl.ds(al((q // 2) * W, W), W)], 0, 0)
        up_store(q).start()

    def second_norm(q):
        rows = pl.ds(al(q * 64, 64), 64)
        upstream = part[rows, :] + land[rows, :]
        normed = (stream_one[rows, :] - mean_two[rows, 0:1]) * inv_two[rows, 0:1]
        low = two_low[rows, :].astype(f32)
        down_sum[0:1, :] = down_sum[0:1, :] + jnp.sum(low, axis=0, keepdims=True)
        grad = low + norm_back(upstream, normed, inv_two[rows, 0:1], gains[1:2, :])
        grad_one[rows, :] = grad
        one_low[rows, :] = grad.astype(bf16)
        add_sum(0, grad)
        add_sum(1, upstream * normed)
        add_sum(2, upstream)

    def into_heads(q):
        rows = pl.ds(al(q * 128, 128), 128)
        grad_att[rows, :] = mm(one_low[rows, :], out_w[...], 1, 1).astype(bf16)

    def attention(q):
        image, pair = q // 4, lax.rem(q, 4)
        rows, cols = pl.ds(al(image * slots, slots), slots), pl.ds(al(pair * 128, 128), 128)
        qs, ks, vs, gs = queries[rows, cols], keys[rows, cols], values[rows, cols], grad_att[rows, cols]
        keep = lax.broadcasted_iota(jnp.int32, (1, slots), 1) < lens[image]
        scale = 1.0 / math.sqrt(HD)
        dq, dk, dv = [], [], []
        for h in range(2):
            part_of = slice(h * HD, (h + 1) * HD)
            qh, kh, vh, gh = qs[:, part_of], ks[:, part_of], vs[:, part_of], gs[:, part_of]
            scores = jnp.where(keep, mm(qh, kh, 1, 1) * scale, -1e30)
            exps = jnp.exp(scores - jnp.max(scores, axis=-1, keepdims=True))
            probs = exps / jnp.sum(exps, axis=-1, keepdims=True)
            grad_probs = mm(gh, vh, 1, 1)
            dv.append(mm(probs.astype(bf16), gh, 0, 0))
            dot = jnp.sum(probs * grad_probs, axis=-1, keepdims=True)
            grad_scores = (probs * (grad_probs - dot)).astype(bf16)
            dq.append(mm(grad_scores, kh, 1, 0) * scale)
            dk.append(mm(grad_scores, qh, 0, 0) * scale)
        for at, pieces in enumerate((dq, dk, dv)):
            grad_proj[at, rows, cols] = jnp.concatenate(pieces, axis=1).astype(bf16)

    def into_norm(q):
        rows = pl.ds(al(q * 128, 128), 128)
        part[rows, :] = (
            mm(grad_proj[0, rows, :], qkv_w[0], 1, 1)
            + mm(grad_proj[1, rows, :], qkv_w[1], 1, 1)
            + mm(grad_proj[2, rows, :], qkv_w[2], 1, 1))

    def out_weight(q):
        cols = pl.ds(al(q * 128, 128), 128)
        tall[0:128, :] = mm(attended[:, cols], one_low[...], 0, 0)
        out_store(q).start()

    def proj_weight(q):
        which, block = q // 4, lax.rem(q, 4)
        cols = pl.ds(al(block * 256, 256), 256)
        wide[0:256, :] = mm(attn_in[:, cols], grad_proj[which], 0, 0)
        proj_store(q).start()

    def first_norm(q):
        rows = pl.ds(al(q * 64, 64), 64)
        upstream, normed = part[rows, :] + land_two[rows, :], normed_one[rows, :]
        grad = grad_one[rows, :] + norm_back(upstream, normed, inv_one[rows, 0:1], gains[0:1, :])
        zero_low[rows, :] = grad.astype(bf16)
        add_sum(3, upstream * normed)
        add_sum(4, upstream)
        add_sum(5, grad)

    def embed_weight(q):
        cols = pl.ds(al(q * 256, 256), 256)
        tall[...] = mm(pixel_low[:, cols], zero_low[...], 0, 0)
        embed_store(q).start()

    def pixels_back(q):
        rows = pl.ds(al(q * 128, 128), 128)
        grad = mm(zero_low[rows, :], embed_w[...], 1, 1)
        grad_pix[rows, :] = grad
        add_sum(6, grad)
        add_sum(7, grad * pixel_hat[rows, :])

    def pack(q):
        for col in range(blocks):
            small_grad[col : col + 1, :] = up_sum[0:1, col * W : (col + 1) * W]
        for col in range(2):
            small_grad[4 + col : 5 + col, :] = down_sum[0:1, col * W : (col + 1) * W]
        for row in range(8):
            small_grad[8 + 2 * row : 9 + 2 * row, :] = sums[row : row + 1, :W]
            small_grad[9 + 2 * row : 10 + 2 * row, :] = sums[row : row + 1, W:]
        for row, at in ((24, 0), (25, 2)):
            small_grad[row : row + 1, :] = jnp.sum(grad_proj[at].astype(f32), axis=0, keepdims=True)

    def keep_rows(q, height):
        at = lax.rem(q, slots // height) * height + lax.broadcasted_iota(jnp.int32, (height, 1), 0)
        return (at < lens[q // (slots // height)]).astype(f32)

    def layer_end(q):
        rows = pl.ds(al(q * 64, 64), 64)
        total_row = stream_one[rows, :] + (mlp_part[rows, :] + land[rows, :]) + down_bias[...]
        one_low[rows, :] = (total_row * keep_rows(q, 64)).astype(bf16)

    def pixel_end(q):
        rows = pl.ds(al(q * 128, 128), 128)
        keep = keep_rows(q, 128)
        first = jnp.concatenate([small_total[20:21, :], small_total[21:22, :]], axis=1)
        cross = jnp.concatenate([small_total[22:23, :], small_total[23:24, :]], axis=1)
        band = pixel_hat.shape[1] // 3
        for at in range(3):
            cols = slice(at * band, (at + 1) * band)
            a_sum = jnp.sum(first[:, cols], axis=1, keepdims=True)
            b_sum = jnp.sum(cross[:, cols], axis=1, keepdims=True)
            grad_pix[rows, cols] = stats[1:2, cols] * (
                grad_pix[rows, cols]
                - keep * (a_sum + b_sum * pixel_hat[rows, cols]) / stats[2:3, cols])

    def fetch_early(q):
        for at in range(12):
            fetches[at].wait()
        zero_low[...] = land_two[...].astype(bf16)

    def fetch_late(q):
        for at in range(12, FETCH - 1):
            fetches[at].wait()

    def act(method, *copies):
        def piece(q):
            for copy in copies:
                getattr(copy, method)()
        return piece

    def landed(store):
        return lambda q: store(q).wait()

    def shift(piece, by):
        return lambda q: piece(q + by)

    def weights(begin, number, piece, store, base=0):
        return (
            (begin + 1, number, shift(landed(store), base)), (begin, number, shift(piece, base)))

    plan = (
        (0, 1, fetch_early), (0, 4, project), (0, 4, feed),
        *weights(4, 2, down_weight, down_store), *weights(4, 2, up_weight, up_store),
        (7, 12, shift(feed, 4)), (19, 1, act("start", *first_sum)),
        *weights(19, 2, down_weight, down_store, 2), *weights(21, 2, up_weight, up_store, 2),
        *weights(23, 2, down_weight, down_store, 4), *weights(25, 2, up_weight, up_store, 4),
        *weights(27, 2, down_weight, down_store, 6), *weights(29, 2, up_weight, up_store, 6),
        (30, 1, fetch_late), (31, 1, act("wait", first_sum[0])), (31, 4, second_norm),
        (35, 2, into_heads), (37, 4, attention), (41, 2, into_norm),
        (42, 1, act("wait", first_sum[1])), (42, 4, shift(second_norm, 4)),
        (43, 1, act("start", second_sum[0])),
        (46, 2, shift(into_heads, 2)), (48, 4, shift(attention, 4)), (52, 2, shift(into_norm, 2)),
        (54, 1, act("start", second_sum[1])),
        (55, 1, act("wait", second_sum[0])), (55, 4, first_norm),
        *weights(56, 4, out_weight, out_store), *weights(58, 12, proj_weight, proj_store),
        (67, 1, act("wait", second_sum[1])), (67, 4, shift(first_norm, 4)),
        (68, 1, act("start", third_sum)),
        *weights(71, 3, embed_weight, embed_store), (75, 4, pixels_back), (79, 1, pack),
        (93, 1, act("wait", third_sum)), (93, 8, layer_end), (101, 1, act("start", layer_copy)),
        (117, 1, act("start", total_copy)), (118, 1, act("wait", total_copy)), (119, 4, pixel_end),
        (123, 1, act("start", pixel_copy)))
    first = 7
    per_block = 2 * (W // (2 * R)) * 2
    starts, total = [0, 0], 2 * per_block * blocks // 2
    for rows_of, cols_of in shapes[2:]:
        starts.append(total)
        total += (rows_of // (2 * R)) * (cols_of // W)
    NC = total

    def slot(j): return lax.rem(j, K)
    a_mine = al(x*Q, Q); a_other = al((1-x)*Q, Q)
    e_near = al(side*E, E); e_far = al((1-side)*E, E)
    b_near = al(H + side*Q, Q); b_far = al(H + (1-side)*Q, Q)
    aN = al(x*Q + side*E, E); aF = al(x*Q + (1-side)*E, E)
    def hbm(ref, a, j, half):
        if a == 0:
            block, q = j // per_block, lax.rem(j, per_block) - per_block // 2
            r, col = q * (2 * R) + half * R, block * W
        elif a == 1:
            block, q = j // per_block, lax.rem(j, per_block)
            r, col = block * W + (q // 2) * (2 * R) + half * R, lax.rem(q, 2) * W
        else:
            cols = shapes[a][1] // W
            q = j - starts[a]
            r, col = (q // cols) * (2 * R) + half * R, lax.rem(q, cols) * W
        return ref.at[pl.ds(al(r, R), R), pl.ds(al(col, W), W)]
    def rc(kind, src, dst, dev, s):
        k = SEND.index(kind)
        return pltpu.make_async_remote_copy(src_ref=src, dst_ref=dst, send_sem=ssem.at[k, s], recv_sem=rsem.at[k, s], device_id=dev, device_id_type=MESH)
    def desc(kind, j):
        s = slot(j)
        if kind == "x": return rc(kind, own.at[s, pl.ds(a_other, Q)], xl.at[s], dev_x, s)
        if kind == "ob": return rc(kind, own.at[s, pl.ds(H, H)], ob.at[s], dev_o, s)
        if kind == "oa": return rc(kind, ab.at[s], oa.at[s], dev_o, s)
        if kind == "ja": return rc(kind, ab.at[s, pl.ds(e_far, E)], ja.at[s], dev_j, s)
        if kind == "jb": return rc(kind, own.at[s, pl.ds(b_far, Q)], jb.at[s], dev_j, s)
        if kind == "xb": return rc(kind, nbuf.at[s], xbl.at[s], dev_x, s)
        if kind in ("ga", "na"):
            return rc(kind, fin.at[s, pl.ds(aN, E)], fin.at[s, pl.ds(aN, E)], dev_j if kind == "ga" else dev_o, s)
        if kind == "fa": return rc(kind, fin.at[s, pl.ds(aF, E)], fin.at[s, pl.ds(aF, E)], dev_o, s)
        if kind in ("gb", "nb"):
            return rc(kind, fin.at[s, pl.ds(b_near, Q)], fin.at[s, pl.ds(b_near, Q)], dev_j if kind == "gb" else dev_o, s)
        if kind == "fb": return rc(kind, fin.at[s, pl.ds(b_far, Q)], fin.at[s, pl.ds(b_far, Q)], dev_o, s)
        if kind == "xg": return rc(kind, fin.at[s, pl.ds(a_mine, Q)], fin.at[s, pl.ds(a_mine, Q)], dev_x, s)
        if kind == "c": return rc(kind, ins[0].at[pl.ds(0, R), pl.ds(0, W)], cl.at[s], dev_c, s)
        if kind == "cg": return rc(kind, fin.at[s], outs[0].at[pl.ds(0, R), pl.ds(0, W)], dev_c, s)
        raise ValueError(kind)
    def each(j, f):
        for a in range(n):
            if a < 2:
                late = lax.rem(j, per_block) >= per_block // 2
                cond = (j < starts[2]) & (late if a == 0 else jnp.logical_not(late))
            else:
                cond = (j >= starts[a]) & (j < (starts[a + 1] if a + 1 < n else NC))
            pl.when(cond)(functools.partial(f, a))
    d = delays
    def step(tt, carry):
        js = [tt - first - dd for dd in d]
        def on(k): return (js[k] >= 0) & (js[k] < NC)
        @pl.when(on(7))
        def _():
            j = js[7]; s = slot(j)
            pltpu.make_async_copy(fin.at[s], outs[0].at[pl.ds(0, R), pl.ds(0, W)], lsem.at[1, s]).wait()
            desc("cg", j).wait_send(); desc("cg", j).wait_recv()
            desc("c", j).wait_send(); desc("x", j).wait_send(); desc("xg", j).wait_send()
            @pl.when(outer)
            def _():
                desc("oa", j).wait_send(); desc("ob", j).wait_send()
            @pl.when(inner)
            def _():
                for k in ("ja","jb","xb","ga","gb","na","fa","nb","fb"): desc(k, j).wait_send()
        @pl.when(on(6))
        def _():
            j = js[6]
            desc("xg", j).wait_recv()
            @pl.when(outer)
            def _():
                desc("nb", j).wait_recv(); desc("fb", j).wait_recv()
        @pl.when(on(5))
        def _():
            j = js[5]
            @pl.when(inner)
            def _():
                desc("ga", j).wait_recv(); desc("gb", j).wait_recv()
        j5o = tt - first - d[5] - d[8]
        on5o = (j5o >= 0) & (j5o < NC)
        @pl.when(on5o & outer)
        def _():
            desc("na", j5o).wait_recv(); desc("fa", j5o).wait_recv()
        @pl.when(on(4))
        def _():
            j = js[4]; s = slot(j)
            @pl.when(inner)
            def _():
                desc("ja", j).wait_recv(); desc("xb", j).wait_recv()
                fin[s, pl.ds(aN, E)] = ab[s, pl.ds(e_near, E)] + ja[s]
                fin[s, pl.ds(b_near, Q)] = nbuf[s] + xbl[s]
        @pl.when(on(3))
        def _():
            j = js[3]; s = slot(j)
            @pl.when(inner)
            def _():
                desc("oa", j).wait_recv(); desc("jb", j).wait_recv()
                ab[s] = ab[s] + oa[s]
                nbuf[s] = own[s, pl.ds(b_near, Q)] + jb[s]
        @pl.when(on(2))
        def _():
            j = js[2]; s = slot(j)
            desc("x", j).wait_recv()
            ab[s] = own[s, pl.ds(a_mine, Q)] + xl[s]
            @pl.when(inner)
            def _():
                desc("ob", j).wait_recv()
                own[s, pl.ds(H, H)] = own[s, pl.ds(H, H)] + ob[s]
        @pl.when(on(1))
        def _():
            j = js[1]; s = slot(j)
            pltpu.make_async_copy(ins[0].at[pl.ds(0, R), pl.ds(0, W)], own.at[s], lsem.at[0, s]).wait()
            desc("c", j).wait_recv()
            own[s] = own[s] + cl[s]
        @pl.when(on(6))
        def _():
            j = js[6]; s = slot(j)
            def f(a):
                pltpu.make_async_copy(fin.at[s], hbm(outs[a], a, j, c), lsem.at[1, s]).start()
                rc("cg", fin.at[s], hbm(outs[a], a, j, c), dev_c, s).start()
            each(j, f)
        @pl.when(on(5))
        def _():
            j = js[5]
            @pl.when(inner)
            def _():
                desc("fa", j).start(); desc("xg", j).start(); desc("fb", j).start()
        @pl.when(on5o & outer)
        def _():
            desc("xg", j5o).start()
        @pl.when(on(4))
        def _():
            j = js[4]
            @pl.when(inner)
            def _():
                for k in ("ga","na","gb","nb"): desc(k, j).start()
        @pl.when(on(3))
        def _():
            j = js[3]
            @pl.when(inner)
            def _():
                desc("ja", j).start(); desc("xb", j).start()
        @pl.when(on(2))
        def _():
            j = js[2]
            @pl.when(outer)
            def _(): desc("oa", j).start()
            @pl.when(inner)
            def _(): desc("jb", j).start()
        @pl.when(on(1))
        def _():
            j = js[1]
            desc("x", j).start()
            @pl.when(outer)
            def _(): desc("ob", j).start()
        @pl.when(on(0))
        def _():
            j = js[0]; s = slot(j)
            def f(a):
                pltpu.make_async_copy(hbm(ins[a], a, j, c), own.at[s], lsem.at[0, s]).start()
                rc("c", hbm(ins[a], a, j, 1 - c), cl.at[s], dev_c, s).start()
            each(j, f)
        for begin, number, piece in plan:
            if number == 1:
                pl.when(tt == begin)(functools.partial(piece, 0))
            else:
                pl.when((tt >= begin) & (tt < begin + number))(functools.partial(piece, tt - begin))
        return carry
    lax.fori_loop(0, first + NC + d[7], step, 0)
    layer_copy.wait()
    pixel_copy.wait()


def back_pass(lengths, fetched, R=64, K=14, delays=(0, 1, 3, 5, 7, 9, 12, 13, 1)):
    f32, bf16 = jnp.float32, jnp.bfloat16
    tokens, width = fetched[2].shape
    hidden = fetched[6].shape[1]
    local = fetched[0].shape[1]
    patch = fetched[17].shape[1]
    shapes = (
        (width, hidden), (hidden, width), (local, width), (3 * width, local), (2 * R, W), (patch, width))
    n = len(shapes)
    H, Q, E = R // 2, R // 4, R // 8
    V = lambda r: pltpu.VMEM((K, r, W), f32)
    anywhere = pl.BlockSpec(memory_space=pl.ANY)
    held = [pltpu.VMEM(a.shape, a.dtype) for a in fetched[:-3]]
    out = [jax.ShapeDtypeStruct(s, f32) for s in shapes]
    out += [jax.ShapeDtypeStruct(s, f32) for s in shapes[:4] + shapes[5:]]
    out += [jax.ShapeDtypeStruct((tokens, width), bf16), jax.ShapeDtypeStruct((tokens, patch), f32)]
    stream = pltpu.VMEM((tokens, width), f32)
    narrow = pltpu.VMEM((tokens, width), bf16)
    results = pl.pallas_call(
        functools.partial(back_kernel, shapes, R, K, delays),
        out_shape=out,
        in_specs=[pl.BlockSpec(memory_space=pltpu.SMEM)] + [anywhere] * FETCH,
        out_specs=[anywhere] * len(out),
        scratch_shapes=[
            *held,
            stream, stream, stream, stream, stream, narrow, narrow,
            pltpu.VMEM((tokens, local), bf16), pltpu.VMEM((3, tokens, local), bf16),
            pltpu.VMEM((tokens, patch), f32), pltpu.VMEM((tokens, hidden), bf16),
            pltpu.VMEM((tokens, hidden), bf16), pltpu.VMEM((8, width), f32),
            pltpu.VMEM((1, hidden), f32), pltpu.VMEM((1, width), f32), pltpu.VMEM(shapes[4], f32),
            pltpu.VMEM((32, W), f32), pltpu.VMEM((256, width), f32), pltpu.VMEM((512, W), f32),
            pltpu.VMEM((tokens, local), f32), narrow, pltpu.VMEM((tokens, 128), f32), pltpu.VMEM((tokens, 128), f32),
            V(R), V(R), V(Q), V(Q), V(Q), V(H), V(E), V(Q), V(Q), V(Q), V(R),
            pltpu.SemaphoreType.DMA((len(SEND), K)), pltpu.SemaphoreType.DMA((len(SEND), K)),
            pltpu.SemaphoreType.DMA((2, K)), pltpu.SemaphoreType.DMA((FETCH,)),
            pltpu.SemaphoreType.DMA((8,)), pltpu.SemaphoreType.DMA((9,)), pltpu.SemaphoreType.DMA((9,)),
        ],
        compiler_params=pltpu.CompilerParams(
            collective_id=1, has_side_effects=True, vmem_limit_bytes=67_000_000),
        name="back_pass")(lengths, *fetched)
    return (*results[:n], *results[-2:])


def stats_kernel(ranks, band_width, lens, pix, out, mine, table, ssem, rsem):
    me = lax.axis_index("dp")
    t = lax.axis_index("tensor")
    bar = pltpu.get_barrier_semaphore()
    for k in range(1, ranks):
        pl.semaphore_signal(bar, inc=1, device_id=(lax.rem(me + k, ranks), t), device_id_type=MESH)
    images, slots, width = pix.shape
    one = jnp.zeros((1, width), jnp.float32)
    two = jnp.zeros((1, width), jnp.float32)
    number = jnp.zeros((1, width), jnp.float32)
    for k in range(images):
        keep = (lax.broadcasted_iota(jnp.int32, (slots, 1), 0) < lens[k]).astype(jnp.float32)
        x = pix[k].astype(jnp.float32)
        kept = x * keep
        one = one + jnp.sum(kept, axis=0, keepdims=True)
        two = two + jnp.sum(kept * x, axis=0, keepdims=True)
        number = number + jnp.sum(keep, axis=0, keepdims=True)
    folded = []
    for line in (one, two):
        for b in range(3):
            at = b * band_width
            folded.append(
                sum(line[:, at + lane : at + lane + 128] for lane in range(0, band_width, 128)))
    folded += [number[:, :128], jnp.zeros((1, 128), jnp.float32)]
    mine[...] = jnp.concatenate(folded, axis=0)
    pl.semaphore_wait(bar, ranks - 1)

    def copy(k):
        peer = lax.rem(me + k, ranks)
        return pltpu.make_async_remote_copy(
            src_ref=mine, dst_ref=table.at[me], send_sem=ssem.at[k - 1], recv_sem=rsem.at[me],
            device_id=(peer, t), device_id_type=MESH)

    def arrival(k):
        peer = lax.rem(me + k, ranks)
        return pltpu.make_async_remote_copy(
            src_ref=mine, dst_ref=table.at[peer], send_sem=ssem.at[k - 1], recv_sem=rsem.at[peer],
            device_id=(peer, t), device_id_type=MESH)

    for k in range(1, ranks):
        copy(k).start()
    table[me] = mine[...]
    for k in range(1, ranks):
        arrival(k).wait_recv()
    total = table[0]
    for k in range(1, ranks):
        total = total + table[k]
    for k in range(1, ranks):
        copy(k).wait_send()
    for b in range(width // band_width):
        cols = slice(b * band_width, (b + 1) * band_width)
        count = jnp.concatenate([total[6:7, :]] * (band_width // 128), axis=1) * float(band_width)
        mean = jnp.sum(total[b : b + 1, :], axis=1, keepdims=True) / count
        square = jnp.sum(total[3 + b : 4 + b, :], axis=1, keepdims=True) / count
        rstd = lax.rsqrt(square - mean * mean + 1e-05)
        out[:, cols] = jnp.concatenate(
            [mean, rstd, count, jnp.zeros((5, band_width), jnp.float32)], axis=0)


def band_stats(pixels, lengths, ranks):
    width = pixels.shape[2]
    return pl.pallas_call(
        functools.partial(stats_kernel, ranks, width // 3),
        out_shape=jax.ShapeDtypeStruct((8, width), jnp.float32),
        in_specs=[pl.BlockSpec(memory_space=pltpu.SMEM), pl.BlockSpec(memory_space=pltpu.VMEM)],
        out_specs=pl.BlockSpec(memory_space=pltpu.VMEM),
        scratch_shapes=[
            pltpu.VMEM((8, 128), jnp.float32),
            pltpu.VMEM((ranks, 8, 128), jnp.float32),
            pltpu.SemaphoreType.DMA((ranks,)),
            pltpu.SemaphoreType.DMA((ranks,)),
        ],
        compiler_params=pltpu.CompilerParams(collective_id=2, has_side_effects=True),
        name="band_stats")(lengths, pixels)


def heads_kernel(lens, attn_in, qkv_w, bias, queries, keys, values, attended, wide):
    f32, bf16 = jnp.float32, jnp.bfloat16
    slots = attn_in.shape[0] // lens.shape[0]

    def mm(a, b, ca, cb):
        return lax.dot_general(a, b, (((ca,), (cb,)), ((), ())), preferred_element_type=f32)

    queries[...] = (mm(attn_in[...], qkv_w[0], 1, 0) + bias[0:1, :]).astype(bf16)
    keys[...] = mm(attn_in[...], qkv_w[1], 1, 0).astype(bf16)
    values[...] = (mm(attn_in[...], qkv_w[2], 1, 0) + bias[1:2, :]).astype(bf16)
    pairs = queries.shape[1] // 128

    def piece(q, carry):
        image, pair = q // pairs, lax.rem(q, pairs)
        rows = pl.ds(pl.multiple_of(image * slots, slots), slots)
        cols = pl.ds(pl.multiple_of(pair * 128, 128), 128)
        qs, ks, vs = queries[rows, cols], keys[rows, cols], values[rows, cols]
        keep = lax.broadcasted_iota(jnp.int32, (1, slots), 1) < lens[image]
        heads = []
        for h in range(2):
            at = slice(h * HD, (h + 1) * HD)
            scores = mm(qs[:, at], ks[:, at], 1, 1) * (1.0 / math.sqrt(HD))
            scores = jnp.where(keep, scores, -1e30)
            exps = jnp.exp(scores - jnp.max(scores, axis=-1, keepdims=True))
            probs = exps / jnp.sum(exps, axis=-1, keepdims=True)
            heads.append(mm(probs.astype(bf16), vs[:, at], 1, 0))
        joined = jnp.concatenate(heads, axis=1).astype(bf16)
        attended[rows, cols] = joined
        wide[rows, cols] = joined.astype(f32)
        return carry

    lax.fori_loop(0, lens.shape[0] * pairs, piece, 0)


def heads_forward(lengths, attn_in, qkv_w, bias):
    tokens, local = attn_in.shape[0], qkv_w.shape[2]
    vmem = pl.BlockSpec(memory_space=pltpu.VMEM)
    low = jax.ShapeDtypeStruct((tokens, local), jnp.bfloat16)
    return pl.pallas_call(
        heads_kernel,
        out_shape=[low, low, low, low, jax.ShapeDtypeStruct((tokens, local), jnp.float32)],
        in_specs=[pl.BlockSpec(memory_space=pltpu.SMEM), vmem, vmem, vmem],
        out_specs=[vmem] * 5,
        compiler_params=pltpu.CompilerParams(vmem_limit_bytes=32 << 20),
        name="heads_forward")(lengths, attn_in, qkv_w, bias)


def positions(patch_ids, gsd_values, model_width, grid_side):
    quarter = model_width // 4
    gsd_scale = gsd_values.astype(jnp.float32) / 100.0
    row_pos = (patch_ids // grid_side).astype(jnp.float32) * gsd_scale[:, None]
    col_pos = (patch_ids % grid_side).astype(jnp.float32) * gsd_scale[:, None]
    frequency = jnp.exp(jnp.arange(quarter, dtype=jnp.float32) * (-math.log(10000.0) / quarter))
    row_angle = row_pos[:, :, None] * frequency
    col_angle = col_pos[:, :, None] * frequency
    return jnp.concatenate(
        [jnp.sin(row_angle), jnp.cos(row_angle), jnp.sin(col_angle), jnp.cos(col_angle)], axis=-1
    )


def contract_rows(left_side, right_side):
    return lax.dot_general(
        left_side, right_side, (((0,), (0,)), ((), ())), preferred_element_type=jnp.float32
    )


def contract_cols(left_side, right_side):
    return lax.dot_general(
        left_side, right_side, (((1,), (1,)), ((), ())), preferred_element_type=jnp.float32
    )


def normalize(hidden, gain_row, shift_row):
    centred = hidden - jnp.mean(hidden, axis=-1, keepdims=True)
    inverse = lax.rsqrt(jnp.mean(centred * centred, axis=-1, keepdims=True) + 1e-06)
    normed = centred * inverse
    return (normed * gain_row + shift_row, normed, inverse)


def normalize_back(upstream, normed, inverse, gain_row):
    scaled = upstream * gain_row
    return inverse * (
        scaled
        - jnp.mean(scaled, axis=-1, keepdims=True)
        - normed * jnp.mean(scaled * normed, axis=-1, keepdims=True)
    )


def gelu_slope(inputs):
    return 0.5 * (1.0 + lax.erf(inputs * (1.0 / math.sqrt(2.0)))) + inputs * jnp.exp(
        -0.5 * inputs * inputs
    ) * (1.0 / math.sqrt(2.0 * math.pi))


def tensor_sum(part):
    if lax.axis_size("tensor") != 2:
        return lax.psum(part, "tensor")
    return part + lax.ppermute(part, "tensor", [(0, 1), (1, 0)])


def per_device(
    fast,
    pixels,
    lengths,
    patch_ids,
    gsd_values,
    embed_w,
    embed_bias,
    norm_gain,
    norm_bias,
    qkv_w,
    qv_bias,
    out_w,
    out_bias,
    up_w,
    up_bias,
    down_w,
    down_bias,
    cotangent,
):
    images, slot_count, patch_width = pixels.shape
    band_width = patch_width // 3
    model_width = embed_w.shape[1]
    local_width = qkv_w.shape[2]
    head_dim = HD
    heads_here = local_width // head_dim
    tokens = images * slot_count
    score_scale = 1.0 / math.sqrt(head_dim)
    key_keep = jnp.arange(slot_count)[None, :] < lengths[:, None]
    valid_rows = key_keep.astype(jnp.float32)
    pixel_grid = pixels.astype(jnp.float32).reshape(images, slot_count, 3, band_width)
    pixel_mask = valid_rows[:, :, None, None]
    if fast:
        half = local_width // 2
        core = lax.rem(lax.axis_index("dp"), 2)
        near_w = lax.dynamic_slice_in_dim(out_w, core * half, half, 0).astype(jnp.float32)
        near_w = lax.ppermute(near_w, "tensor", [(0, 1), (1, 0)])
        mate_w = lax.ppermute(near_w, "dp", [(k, k ^ 1) for k in range(16)])
        stats = band_stats(pixels, lengths, 16)
        band_mean = stats[0].reshape(3, band_width)[:, 0]
        band_rstd = stats[1].reshape(3, band_width)[:, 0]
        band_count = stats[2, 0]
    else:
        total_one, total_two, band_count = lax.psum(
            (
                jnp.sum(pixel_grid * pixel_mask, axis=(0, 1, 3)),
                jnp.sum(pixel_grid * pixel_grid * pixel_mask, axis=(0, 1, 3)),
                jnp.sum(valid_rows) * band_width,
            ),
            "dp",
        )
        band_mean = total_one / band_count
        band_rstd = lax.rsqrt(total_two / band_count - band_mean * band_mean + 1e-05)
    pixel_hat = (pixel_grid - band_mean[:, None]) * band_rstd[:, None]
    pixel_low = pixel_hat.reshape(tokens, patch_width).astype(jnp.bfloat16)
    pos_table = positions(patch_ids, gsd_values, model_width, GRID).reshape(tokens, model_width)
    stream_zero = (
        jnp.dot(pixel_low, embed_w, preferred_element_type=jnp.float32) + embed_bias + pos_table
    )
    layer_one, normed_one, inverse_one = normalize(stream_zero, norm_gain[0], norm_bias[0])
    attn_input = layer_one.astype(jnp.bfloat16)
    if fast:
        row_valid = valid_rows.reshape(tokens, 1)
        queries, key_rows, values, attended, att_wide = heads_forward(lengths, attn_input, qkv_w, qv_bias)
        spread = lambda column: jnp.broadcast_to(column, (tokens, 128))
        two_low = cotangent.reshape(tokens, model_width) * row_valid.astype(jnp.bfloat16)
        fetched = (
            attended, out_w, stream_zero, norm_gain, norm_bias, out_bias.reshape(1, -1), up_w, down_w,
            up_bias.reshape(1, -1), two_low, queries, key_rows, values, attn_input, qkv_w, normed_one,
            spread(inverse_one), pixel_low, pixel_hat.reshape(tokens, patch_width), embed_w,
            down_bias.reshape(1, -1), stats, att_wide, near_w, mate_w)
        sum_up, sum_down, sum_out_proj, sum_qkv, small, embed_sum, output, pixel_grad = back_pass(
            lengths, fetched)
        rows = small[8:24].reshape(8, 2 * W)
        return (
            output.reshape(images, slot_count, model_width),
            pixel_grad.reshape(images, slot_count, patch_width),
            embed_sum,
            rows[5],
            jnp.stack([rows[3], rows[1]]),
            jnp.stack([rows[4], rows[2]]),
            sum_qkv.reshape(3, model_width, local_width),
            small[24:26],
            sum_out_proj,
            rows[0],
            sum_up,
            small[0:4].reshape(-1),
            sum_down,
            small[4:6].reshape(-1),
        )
    queries = (
        jnp.dot(attn_input, qkv_w[0], preferred_element_type=jnp.float32) + qv_bias[0]
    ).astype(jnp.bfloat16)
    key_rows = jnp.dot(attn_input, qkv_w[1], preferred_element_type=jnp.float32).astype(
        jnp.bfloat16
    )
    values = (
        jnp.dot(attn_input, qkv_w[2], preferred_element_type=jnp.float32) + qv_bias[1]
    ).astype(jnp.bfloat16)
    query_heads = queries.reshape(images, slot_count, heads_here, head_dim)
    key_heads = key_rows.reshape(images, slot_count, heads_here, head_dim)
    value_heads = values.reshape(images, slot_count, heads_here, head_dim)

    def score_block():
        scores = (
            jnp.einsum(
                "ichd,ijhd->ihcj", query_heads, key_heads, preferred_element_type=jnp.float32
            )
            * score_scale
        )
        return jnp.where(key_keep[:, None, None, :], scores, -1e30)

    scores = score_block()
    top_score = jnp.max(scores, axis=-1, keepdims=True)
    exp_scores = jnp.exp(scores - top_score)
    exp_total = jnp.sum(exp_scores, axis=-1, keepdims=True)
    log_total = top_score + jnp.log(exp_total)
    prob_low = (exp_scores / exp_total).astype(jnp.bfloat16)
    attended = (
        jnp.einsum("ihcj,ijhd->ichd", prob_low, value_heads, preferred_element_type=jnp.float32)
        .astype(jnp.bfloat16)
        .reshape(tokens, local_width)
    )
    attn_out = tensor_sum(jnp.dot(attended, out_w, preferred_element_type=jnp.float32))
    stream_one = stream_zero + attn_out + out_bias
    layer_two, normed_two, inverse_two = normalize(stream_one, norm_gain[1], norm_bias[1])
    mlp_input = layer_two.astype(jnp.bfloat16)
    hidden_pre = jnp.dot(mlp_input, up_w, preferred_element_type=jnp.float32) + up_bias
    hidden_low = jax.nn.gelu(hidden_pre, approximate=False).astype(jnp.bfloat16)
    mlp_part = jnp.dot(hidden_low, down_w, preferred_element_type=jnp.float32)
    row_valid = valid_rows.reshape(tokens, 1)
    grad_two = cotangent.astype(jnp.float32).reshape(tokens, model_width) * row_valid
    grad_down_bias = jnp.sum(grad_two, axis=0)
    grad_two_low = grad_two.astype(jnp.bfloat16)
    grad_down = contract_rows(hidden_low, grad_two_low)
    grad_hidden = (contract_cols(grad_two_low, down_w) * gelu_slope(hidden_pre)).astype(
        jnp.bfloat16
    )
    grad_up = contract_rows(mlp_input, grad_hidden)
    grad_up_bias = jnp.sum(grad_hidden.astype(jnp.float32), axis=0)
    grad_mlp_in = tensor_sum(contract_cols(grad_hidden, up_w))
    grad_one = grad_two + normalize_back(grad_mlp_in, normed_two, inverse_two, norm_gain[1])
    grad_out_bias = jnp.sum(grad_one, axis=0)
    grad_one_low = grad_one.astype(jnp.bfloat16)
    grad_out_proj = contract_rows(attended, grad_one_low)
    grad_attended = (
        contract_cols(grad_one_low, out_w)
        .astype(jnp.bfloat16)
        .reshape(images, slot_count, heads_here, head_dim)
    )
    attn_probs = jnp.exp(score_block() - log_total)
    grad_probs = jnp.einsum(
        "ichd,ijhd->ihcj", grad_attended, value_heads, preferred_element_type=jnp.float32
    )
    grad_values = jnp.einsum(
        "ihcj,ichd->ijhd",
        attn_probs.astype(jnp.bfloat16),
        grad_attended,
        preferred_element_type=jnp.float32,
    ).astype(jnp.bfloat16)
    prob_dot = jnp.sum(attn_probs * grad_probs, axis=-1, keepdims=True)
    grad_scores = (attn_probs * (grad_probs - prob_dot)).astype(jnp.bfloat16)
    grad_queries = (
        jnp.einsum("ihcj,ijhd->ichd", grad_scores, key_heads, preferred_element_type=jnp.float32)
        * score_scale
    ).astype(jnp.bfloat16)
    grad_keys = (
        jnp.einsum("ihcj,ichd->ijhd", grad_scores, query_heads, preferred_element_type=jnp.float32)
        * score_scale
    ).astype(jnp.bfloat16)
    grad_proj = (
        grad_queries.reshape(tokens, local_width),
        grad_keys.reshape(tokens, local_width),
        grad_values.reshape(tokens, local_width),
    )
    grad_qkv = jnp.stack([contract_rows(attn_input, grad_piece) for grad_piece in grad_proj])
    grad_qv_bias = jnp.stack(
        [
            jnp.sum(grad_proj[0].astype(jnp.float32), axis=0),
            jnp.sum(grad_proj[2].astype(jnp.float32), axis=0),
        ]
    )
    attn_partial = (
        contract_cols(grad_proj[0], qkv_w[0])
        + contract_cols(grad_proj[1], qkv_w[1])
        + contract_cols(grad_proj[2], qkv_w[2])
    )
    grad_attn_in = tensor_sum(attn_partial)
    mlp_part, _ = lax.optimization_barrier((mlp_part, grad_attn_in))
    stream_two = stream_one + tensor_sum(mlp_part) + down_bias
    output = (stream_two * row_valid).astype(jnp.bfloat16).reshape(images, slot_count, model_width)
    grad_zero = grad_one + normalize_back(grad_attn_in, normed_one, inverse_one, norm_gain[0])
    grad_norm_gain = jnp.stack(
        [jnp.sum(grad_attn_in * normed_one, axis=0), jnp.sum(grad_mlp_in * normed_two, axis=0)]
    )
    grad_norm_bias = jnp.stack([jnp.sum(grad_attn_in, axis=0), jnp.sum(grad_mlp_in, axis=0)])
    grad_embed_bias = jnp.sum(grad_zero, axis=0)
    grad_zero_low = grad_zero.astype(jnp.bfloat16)
    embed_part = contract_rows(pixel_low, grad_zero_low)
    grad_pixel_hat = contract_cols(grad_zero_low, embed_w).reshape(
        images, slot_count, 3, band_width
    )
    band_grad = jnp.sum(grad_pixel_hat, axis=(0, 1, 3))
    band_cross = jnp.sum(grad_pixel_hat * pixel_hat, axis=(0, 1, 3))
    small = (
        grad_qv_bias,
        grad_out_bias,
        grad_up_bias,
        grad_down_bias,
        grad_norm_gain,
        grad_norm_bias,
        grad_embed_bias,
        band_grad,
        band_cross,
    )
    large = (grad_qkv.reshape(-1, local_width), grad_out_proj, grad_up, grad_down, embed_part)
    large, small = lax.psum((large, small), "dp")
    sum_qkv, sum_out_proj, sum_up, sum_down, embed_sum = large
    sum_qkv = sum_qkv.reshape(grad_qkv.shape)
    (
        sum_qv_bias,
        sum_out_bias,
        sum_up_bias,
        sum_down_bias,
        sum_gain,
        sum_shift,
        sum_embed_bias,
        band_grad_sum,
        band_cross_sum,
    ) = small
    pixel_grad = band_rstd[:, None] * (
        grad_pixel_hat
        - pixel_mask * (band_grad_sum[:, None] + band_cross_sum[:, None] * pixel_hat) / band_count
    )
    pixel_grad = pixel_grad.reshape(images, slot_count, patch_width)
    return (
        output,
        pixel_grad,
        embed_sum,
        sum_embed_bias,
        sum_gain,
        sum_shift,
        sum_qkv,
        sum_qv_bias,
        sum_out_proj,
        sum_out_bias,
        sum_up,
        sum_up_bias,
        sum_down,
        sum_down_bias,
    )


def solution(mesh):
    fast = dict(mesh.shape) == {"dp": 16, "tensor": 2}
    in_specs = (
        P("dp", None, None),
        P("dp"),
        P("dp", None),
        P("dp"),
        P(),
        P(),
        P(),
        P(),
        P(None, None, "tensor"),
        P(None, "tensor"),
        P("tensor", None),
        P(),
        P(None, "tensor"),
        P("tensor"),
        P("tensor", None),
        P(),
        P("dp", None, None),
    )
    out_specs = (
        P("dp", None, None),
        P("dp", None, None),
        P(),
        P(),
        P(),
        P(),
        P(None, None, "tensor"),
        P(None, "tensor"),
        P("tensor", None),
        P(),
        P(None, "tensor"),
        P("tensor"),
        P("tensor", None),
        P(),
    )
    return jax.shard_map(
        functools.partial(per_device, fast), mesh=mesh, in_specs=in_specs, out_specs=out_specs, check_vma=False
    )
```
